128 devices in a mesh: rows: 16 (over x, z_lo, core), planes: 8 (over y, z_hi).
Axes of the slice: x: 4, y: 4, z: 4 (z_hi: 2, z_lo: 2; z = z_hi * 2 + z_lo), core: 2. Of those that a mesh axis runs over, the one named last changes fastest.
Arguments:
- density: float32 [8, 4096, 4096], P('planes', 'rows'), may hold values from -6 to 6
- lens_weight: float32 [8], P('planes'), may hold values from 0.05 to 0.5
- spectrum_bin: int32 [4096, 4096], P(None, ('rows', 'planes')), may hold values from 0 to 63, as said below
Outputs:
- shear_real: float32 [4096, 4096], P(('rows', 'planes'))
- shear_imag: float32 [4096, 4096], P(('rows', 'planes'))
- spectrum: float32 [64], replicated
The draws below stay inside these ranges and needn't reach their ends.
Inputs may be any that keep to these rules, and one draw needn't show every extreme that they name: `spectrum_bin`: each Fourier pixel's band.
All inputs are finite; a program needn't handle non-finite values.
Results may differ from the reference program's by a relative error of at most 0.0003.
Values sent between devices are 32-bit elements; how exact they have to be, the bound alone decides.
No kernel may reach another device: no remote copies, remote signals or barrier semaphores. Data moves between devices by JAX's collectives and lax.ppermute only.
A program may use at most 64 MiB of HBM per device.

```python
import math
import jax
import jax.numpy as jnp
from jax import lax

N = 4096
NBINS = 64
PLANES = 8


def draw_spectrum_bin(key, part):
    frequency = (jnp.arange(N, dtype=jnp.int32) + N // 2) % N - N // 2
    square_norm = frequency[:, None] ** 2 + frequency[None, :] ** 2
    radial = jnp.minimum(square_norm * NBINS // (N * N // 2), NBINS - 1)
    jitter = jax.random.randint(key, (N, N), -1, 2, dtype=jnp.int32)
    return jnp.clip(radial + jitter, 0, NBINS - 1).astype(jnp.int32)


def level_of(rng, shape, cuts, least, high):
    level = 1.0
    for axis_at, parts in cuts:
        draws = jax.random.uniform(jax.random.fold_in(jax.random.fold_in(rng, 6), axis_at), (parts,), jnp.float32, least / len(cuts), high / len(cuts))
        level = level * jnp.repeat(jnp.exp(draws), shape[axis_at] // parts).reshape((-1,) + (1,) * (len(shape) - 1 - axis_at))
    return level


def bell_draw(rng, dims, spread, limit, cuts=(), held_as=jnp.bfloat16):
    entries = spread * jax.random.normal(rng, dims, jnp.float32)
    if cuts:
        entries = entries * level_of(rng, dims, cuts, -0.22, 0.18)
    return jnp.clip(entries, -limit, limit).astype(held_as)


def setup_inputs(seed: int = 0) -> dict:
    keys = jax.random.split(jax.random.key(seed), 4)
    return {
        "density": bell_draw(keys[0], (PLANES, N, N), 1.0, 6.0, ((0, 8), (1, 16)), jnp.float32),
        "lens_weight": jnp.clip(jnp.exp(math.log(0.5) - 2.3025851 * jax.random.uniform(keys[1], (PLANES,), jnp.float32) ** level_of(keys[1], (PLANES,), ((0, 8),), -0.2, 0.2)), 0.05, 0.5),
        "spectrum_bin": draw_spectrum_bin(jax.random.fold_in(keys[3], 71), 0),
    }


def reference(density, lens_weight, spectrum_bin):
    def accumulate(plane_index, running):
        total_real, total_imag = running
        weighted_plane = density[plane_index] * lens_weight[plane_index]
        plane_hat = jnp.fft.fft2(weighted_plane)
        return (total_real + jnp.real(plane_hat), total_imag + jnp.imag(plane_hat))

    empty_sum = jnp.zeros((N, N), jnp.float32)
    total_real, total_imag = lax.fori_loop(0, PLANES, accumulate, (empty_sum, empty_sum))
    frequency = ((jnp.arange(N, dtype=jnp.int32) + N // 2) % N - N // 2).astype(jnp.float32)
    height = frequency[:, None]
    across = frequency[None, :]
    square_norm = height ** 2 + across ** 2
    anchor = square_norm == 0
    safe_norm = jnp.where(anchor, 1.0, square_norm)
    total_real = jnp.where(anchor, 0.0, total_real)
    total_imag = jnp.where(anchor, 0.0, total_imag)
    pixel_power = (total_real ** 2 + total_imag ** 2) * (NBINS / float(N) ** 4)
    spectrum = jax.ops.segment_sum(pixel_power.reshape(-1), spectrum_bin.reshape(-1), num_segments=NBINS)
    kernel_real = (across ** 2 - height ** 2) / safe_norm
    kernel_imag = 2.0 * across * height / safe_norm
    hat_real = kernel_real * total_real - kernel_imag * total_imag
    hat_imag = kernel_real * total_imag + kernel_imag * total_real
    shear_field = jnp.fft.ifft2(hat_real + 1j * hat_imag)
    return jnp.real(shear_field).astype(jnp.float32), jnp.imag(shear_field).astype(jnp.float32), spectrum
```

```python
from functools import partial
import math

import numpy as np
import jax
import jax.numpy as jnp
from jax import lax
from jax.experimental import pallas as pl
from jax.experimental.pallas import tpu as pltpu
from jax.sharding import Mesh
from jax.sharding import PartitionSpec as P

N = 4096
LONG = 128
SHORT = 32
NBINS = 64
ROWS = ("rows_0", "rows_1", "rows_2")
PLANES = ("planes_0", "planes_1")
ROWS_PLANES = ROWS + PLANES
FORTH = 16
BACK = 17
BF16 = jnp.bfloat16


def halves(table):
    high = table.astype(np.float32).astype(jnp.bfloat16)
    low = (table - high.astype(np.float64)).astype(np.float32).astype(jnp.bfloat16)
    return high, low


def tables():
    def wave(left, right, length):
        angle = 2.0 * np.pi * ((left[:, None] * right[None, :]) % length) / length
        return np.cos(angle), np.sin(angle)

    long_index = np.arange(LONG)
    short_index = np.arange(SHORT)
    cos_long, sin_long = wave(long_index, long_index, LONG)
    forth = np.block([[cos_long, sin_long], [-sin_long, cos_long]])
    cos_short, sin_short = wave(short_index, short_index, SHORT)
    cos_four, sin_four = np.kron(np.eye(4), cos_short), np.kron(np.eye(4), sin_short)
    short_forth = np.block([[cos_four, -sin_four], [sin_four, cos_four]])
    row_turn = wave(short_index, long_index, N)
    cos_turn, sin_turn = wave(long_index, short_index, N)
    column_turn = (np.tile(cos_turn, (1, 4)), np.tile(sin_turn, (1, 4)))
    return {
        "forth": np.concatenate(halves(forth), axis=1),
        "back": np.concatenate(halves(forth.T), axis=1),
        "short_forth": np.concatenate(halves(short_forth), axis=0),
        "short_back": np.concatenate(halves(short_forth.T), axis=0),
        "right_back": np.concatenate(halves(forth), axis=0),
        "row_turn": np.stack(row_turn).astype(np.float32),
        "column_turn": np.stack(column_turn).astype(np.float32),
    }


def plus(a, b):
    if a is None:
        return b
    if b is None:
        return a
    return a + b


def minus(a, b):
    if b is None:
        return a
    if a is None:
        return -b
    return a - b


def scaled(a, factor):
    if a is None or factor == 0.0:
        return None
    if factor == 1.0:
        return a
    if factor == -1.0:
        return -a
    return a * factor


def rotated(value, step, length, orient):
    step %= length
    quarter, rest = divmod(4 * step, length)
    real, imag = value
    if rest == 0:
        cosine = (1.0, 0.0, -1.0, 0.0)[quarter]
        sine = (0.0, 1.0, 0.0, -1.0)[quarter] * orient
    else:
        cosine = math.cos(2.0 * math.pi * step / length)
        sine = orient * math.sin(2.0 * math.pi * step / length)
    return (
        minus(scaled(real, cosine), scaled(imag, sine)),
        plus(scaled(real, sine), scaled(imag, cosine)),
    )


def transformed(values, orient):
    length = len(values)
    if length == 1:
        return values
    even = transformed(values[0::2], orient)
    odd = transformed(values[1::2], orient)
    front, rear = [], []
    for k in range(length // 2):
        turned = rotated(odd[k], k, length, orient)
        front.append((plus(even[k][0], turned[0]), plus(even[k][1], turned[1])))
        rear.append((minus(even[k][0], turned[0]), minus(even[k][1], turned[1])))
    return front + rear


def transformed_real(values):
    length = len(values)
    if length == 1:
        return [(values[0], None)]
    if length == 2:
        return [(values[0] + values[1], None), (values[0] - values[1], None)]
    even = transformed_real(values[0::2])
    odd = transformed_real(values[1::2])
    out = [None] * (length // 2 + 1)
    for k in range(length // 4 + 1):
        turned = rotated(odd[k], k, length, -1.0)
        out[k] = (plus(even[k][0], turned[0]), plus(even[k][1], turned[1]))
        mirror_imag = minus(turned[1], even[k][1])
        out[length // 2 - k] = (minus(even[k][0], turned[0]), mirror_imag)
    return out


def split(value):
    high = value.astype(BF16)
    return high, (value - high.astype(jnp.float32)).astype(BF16)


def product(left, right, dims=((1,), (0,))):
    return lax.dot_general(left, right, (dims, ((), ())), preferred_element_type=jnp.float32)


def table_times(table_ref, value):
    size = value.shape[0]
    high, low = split(value)
    stacked = jnp.concatenate([high, low, high], axis=0)
    left = jnp.concatenate([table_ref[:, :size], table_ref[:, :size], table_ref[:, size:]], axis=1)
    return product(left, stacked)


def table_times_rows(table_ref, value):
    size = value.shape[1]
    high, low = split(value)
    stacked = jnp.concatenate([high, low, high], axis=1)
    left = jnp.concatenate([table_ref[:, :size], table_ref[:, :size], table_ref[:, size:]], axis=1)
    return product(left, stacked, ((1,), (1,)))


def times_table(value, table_ref):
    size = value.shape[1]
    high, low = split(value)
    stacked = jnp.concatenate([high, low, high], axis=1)
    right = jnp.concatenate([table_ref[:size], table_ref[:size], table_ref[size:]], axis=0)
    return product(stacked, right)


def rows_forth_kernel(field_ref, turn_ref, forth_ref, out_ref, held_ref):
    for block in range(4):
        rows = slice(8 * block, 8 * block + 8)
        pieces = []
        for n in range(SHORT):
            lanes = slice(LONG * n, LONG * n + LONG)
            total = field_ref[0, rows, lanes]
            for p in range(1, field_ref.shape[0]):
                total = total + field_ref[p, rows, lanes]
            pieces.append(total)
        half = transformed_real(pieces)
        for k in range(SHORT):
            real, imag = half[k] if k <= SHORT // 2 else half[SHORT - k]
            if k > SHORT // 2:
                imag = None if imag is None else -imag
            cosine = turn_ref[0, k : k + 1, :]
            sine = turn_ref[1, k : k + 1, :]
            if imag is None:
                held_ref[k, block, :, :LONG] = real * cosine
                held_ref[k, block, :, LONG:] = -(real * sine)
            else:
                held_ref[k, block, :, :LONG] = real * cosine + imag * sine
                held_ref[k, block, :, LONG:] = imag * cosine - real * sine
    for quarter in range(4):
        rows = held_ref[8 * quarter : 8 * quarter + 8].reshape(256, 2 * LONG)
        spread = table_times_rows(forth_ref, rows)
        for part in range(2):
            for side in range(2):
                tile = 8 * part + 2 * quarter + side
                out_ref[pl.ds(tile, LONG, FORTH), :] = spread[
                    LONG * part : LONG * part + LONG, LONG * side : LONG * side + LONG
                ]


def columns_kernel(
    first_ref,
    arrived_ref,
    bins_ref,
    turn_ref,
    forth_ref,
    back_ref,
    short_forth_ref,
    short_back_ref,
    out_ref,
    power_ref,
    bands_ref,
):
    lane = lax.broadcasted_iota(jnp.int32, (LONG, LONG), 1)
    row = lax.broadcasted_iota(jnp.int32, (LONG, LONG), 0)
    height = row + LONG * (lane % SHORT)
    height = ((height + N // 2) % N - N // 2).astype(jnp.float32)
    height_square = height * height
    first = first_ref[0]
    for pair in range(4):
        columns = []
        for side in range(2):
            group = 2 * pair + side
            columns.append(
                jnp.concatenate(
                    [
                        arrived_ref[pl.ds(group, LONG, FORTH), :],
                        arrived_ref[pl.ds(8 + group, LONG, FORTH), :],
                    ],
                    axis=0,
                )
            )
        spread = table_times(forth_ref, jnp.concatenate(columns, axis=1))
        cosine = turn_ref[0]
        sine = turn_ref[1]
        turned = []
        for side in range(2):
            lanes = slice(LONG * side, LONG * side + LONG)
            real, imag = spread[:LONG, lanes], spread[LONG:, lanes]
            turned.append(
                jnp.concatenate([real * cosine + imag * sine, imag * cosine - real * sine], axis=1)
            )
        held = times_table(jnp.concatenate(turned, axis=0), short_forth_ref)
        hats = []
        for side in range(2):
            group = 2 * pair + side
            real = held[LONG * side : LONG * side + LONG, :LONG]
            imag = held[LONG * side : LONG * side + LONG, LONG:]
            across = first + 4 * group + lane // SHORT
            across = ((across + N // 2) % N - N // 2).astype(jnp.float32)
            across_square = across * across
            square_norm = height_square + across_square
            anchor = square_norm == 0.0
            real = jnp.where(anchor, 0.0, real)
            imag = jnp.where(anchor, 0.0, imag)
            power_ref[LONG * group : LONG * group + LONG, :] = real * real + imag * imag
            inverse = (1.0 / float(N) ** 2) / jnp.where(anchor, 1.0, square_norm)
            kernel_real = (across_square - height_square) * inverse
            kernel_imag = (across * height) * (2.0 * inverse)
            hats.append(
                jnp.concatenate(
                    [
                        kernel_real * real - kernel_imag * imag,
                        kernel_real * imag + kernel_imag * real,
                    ],
                    axis=1,
                )
            )
        returned = times_table(jnp.concatenate(hats, axis=0), short_back_ref)
        columns = []
        for side in range(2):
            rows = slice(LONG * side, LONG * side + LONG)
            real, imag = returned[rows, :LONG], returned[rows, LONG:]
            columns.append(
                jnp.concatenate([real * cosine - imag * sine, imag * cosine + real * sine], axis=0)
            )
        restored = table_times(back_ref, jnp.concatenate(columns, axis=1))
        for part in range(2):
            for side in range(2):
                tile = 8 * part + 2 * pair + side
                out_ref[pl.ds(tile, LONG, BACK), :] = restored[
                    LONG * part : LONG * part + LONG, LONG * side : LONG * side + LONG
                ]

    def one_block(block, carry):
        start = pl.multiple_of(block * 64, 64)
        power = power_ref[pl.ds(start, 64), :]
        bins = bins_ref[pl.ds(start, 64), :]
        for band in range(NBINS):
            chosen = jnp.where(bins == band, power, 0.0)
            bands_ref[8 * band : 8 * band + 8, :] += jnp.sum(chosen.reshape(8, 8, LONG), axis=0)
        return carry

    bands_ref[...] = jnp.zeros_like(bands_ref)
    lax.fori_loop(0, 8 * LONG // 64, one_block, 0)
    sums = jnp.sum(bands_ref[...].reshape(NBINS, 8, LONG), axis=1)
    sums = jnp.concatenate([sums, jnp.zeros((LONG - NBINS, LONG), jnp.float32)], axis=0)
    line = jnp.sum(sums.T, axis=0, keepdims=True) * (NBINS / float(N) ** 4)
    out_ref[pl.ds(16, LONG, BACK), :] = jnp.broadcast_to(line, (LONG, LONG))


def rows_back_kernel(
    arrived_ref, turn_ref, table_ref, real_ref, imag_ref, spectrum_ref, held_ref
):
    for group in range(8):
        pair = jnp.concatenate(
            [
                arrived_ref[pl.ds(group, LONG, BACK), :].T,
                arrived_ref[pl.ds(8 + group, LONG, BACK), :].T,
            ],
            axis=1,
        )
        held_ref[LONG * group : LONG * group + LONG, :] = times_table(pair, table_ref)
    spectrum_ref[...] = jnp.sum(
        arrived_ref[pl.ds(16, LONG, BACK), :], axis=0, keepdims=True
    )
    for block in range(4):
        pieces = []
        for k in range(SHORT):
            rows = slice(SHORT * k + 8 * block, SHORT * k + 8 * block + 8)
            cosine = turn_ref[0, k : k + 1, :]
            sine = turn_ref[1, k : k + 1, :]
            real, imag = held_ref[rows, :LONG], held_ref[rows, LONG:]
            pieces.append((real * cosine - imag * sine, imag * cosine + real * sine))
        for n, (real, imag) in enumerate(transformed(pieces, 1.0)):
            real_ref[8 * block : 8 * block + 8, LONG * n : LONG * n + LONG] = real
            imag_ref[8 * block : 8 * block + 8, LONG * n : LONG * n + LONG] = imag


def call(kernel, outs, scratch, inputs, name, smem_first=False):
    whole = pl.BlockSpec(memory_space=pltpu.VMEM)
    specs = [whole] * len(inputs)
    if smem_first:
        specs[0] = pl.BlockSpec(memory_space=pltpu.SMEM)
    return pl.pallas_call(
        kernel,
        out_shape=outs,
        in_specs=specs,
        out_specs=jax.tree.map(lambda _: whole, outs),
        scratch_shapes=scratch,
        name=name,
        compiler_params=pltpu.CompilerParams(vmem_limit_bytes=48 * 1024 * 1024),
    )(*inputs)


def f32(*shape):
    return jax.ShapeDtypeStruct(shape, jnp.float32)


def exchanged(array, height):
    blocks = array.reshape(LONG, 1, height * LONG)
    blocks = lax.all_to_all(blocks, ROWS_PLANES, split_axis=0, concat_axis=0, tiled=True)
    return blocks.reshape(LONG * height, LONG)


def on_device(density, lens_weight, spectrum_bin):
    held = tables()
    planes_here, slab_rows, length = density.shape
    plane_count = lax.axis_size(PLANES)
    device = lax.axis_index(ROWS_PLANES)
    weighted = density[0] * lens_weight[0]
    blocks = weighted.reshape(plane_count, slab_rows // plane_count, length)
    blocks = lax.all_to_all(blocks, PLANES, split_axis=0, concat_axis=0, tiled=True)
    bins = spectrum_bin.reshape(SHORT, LONG, 8, 4).transpose(2, 1, 3, 0).reshape(8 * LONG, LONG)
    sent = call(
        rows_forth_kernel,
        f32(LONG * FORTH, LONG),
        [pltpu.VMEM((SHORT, 4, 8, 2 * LONG), jnp.float32)],
        (blocks, held["row_turn"], held["forth"]),
        "rows_forth",
    )
    arrived = exchanged(sent, FORTH)
    sent = call(
        columns_kernel,
        f32(LONG * BACK, LONG),
        [pltpu.VMEM((8 * LONG, LONG), jnp.float32), pltpu.VMEM((8 * NBINS, LONG), jnp.float32)],
        (
            (device * SHORT).reshape(1),
            arrived,
            bins,
            held["column_turn"],
            held["forth"],
            held["back"],
            held["short_forth"],
            held["short_back"],
        ),
        "columns",
        smem_first=True,
    )
    arrived = exchanged(sent, BACK)
    shear_real, shear_imag, spectrum = call(
        rows_back_kernel,
        (f32(SHORT, N), f32(SHORT, N), f32(1, LONG)),
        [pltpu.VMEM((8 * LONG, 2 * LONG), jnp.float32)],
        (arrived, held["row_turn"], held["right_back"]),
        "rows_back",
    )
    return shear_real, shear_imag, spectrum[0, :NBINS]


def solution(mesh):
    finer = Mesh(mesh.devices.reshape(4, 2, 2, 4, 2), ROWS_PLANES)
    in_specs = (P(PLANES, ROWS, None), P(PLANES), P(None, ROWS_PLANES))
    out_specs = (P(ROWS_PLANES, None), P(ROWS_PLANES, None), P())
    return jax.shard_map(
        on_device, mesh=finer, in_specs=in_specs, out_specs=out_specs, check_vma=False
    )
```

```python
import math

import numpy as np
import jax
import jax.numpy as jnp
from jax import lax
from jax.experimental import pallas as pl
from jax.experimental.pallas import tpu as pltpu
from jax.sharding import Mesh
from jax.sharding import PartitionSpec as P


N = 4096
LONG = 128
SHORT = 32
NBINS = 64
ROWS = ("rows_0", "rows_1", "rows_2")
PLANES = ("planes_0", "planes_1")
ROWS_PLANES = ROWS + PLANES
FORTH = 16
BACK = 17
EARLY_HALF = 1280
EARLY = 2 * EARLY_HALF
BF16 = jnp.bfloat16


def halves(table):
    high = table.astype(np.float32).astype(jnp.bfloat16)
    low = (table - high.astype(np.float64)).astype(np.float32).astype(jnp.bfloat16)
    return high, low


def tables():
    def wave(left, right, length):
        angle = 2.0 * np.pi * ((left[:, None] * right[None, :]) % length) / length
        return np.cos(angle), np.sin(angle)

    long_index = np.arange(LONG)
    short_index = np.arange(SHORT)
    cos_long, sin_long = wave(long_index, long_index, LONG)
    forth = np.block([[cos_long, sin_long], [-sin_long, cos_long]])
    cos_short, sin_short = wave(short_index, short_index, SHORT)
    cos_four, sin_four = np.kron(np.eye(4), cos_short), np.kron(np.eye(4), sin_short)
    short_forth = np.block([[cos_four, -sin_four], [sin_four, cos_four]])
    row_turn = wave(short_index, long_index, N)
    cos_turn, sin_turn = wave(long_index, short_index, N)
    column_turn = (np.tile(cos_turn, (1, 4)), np.tile(sin_turn, (1, 4)))
    return {
        "forth": np.concatenate(halves(forth), axis=1),
        "back": np.concatenate(halves(forth.T), axis=1),
        "short_forth": np.concatenate(halves(short_forth), axis=0),
        "short_back": np.concatenate(halves(short_forth.T), axis=0),
        "right_back": np.concatenate(halves(forth), axis=0),
        "row_turn": np.stack(row_turn).astype(np.float32),
        "column_turn": np.stack(column_turn).astype(np.float32),
    }


def plus(a, b):
    if a is None:
        return b
    if b is None:
        return a
    return a + b


def minus(a, b):
    if b is None:
        return a
    if a is None:
        return -b
    return a - b


def scaled(a, factor):
    if a is None or factor == 0.0:
        return None
    if factor == 1.0:
        return a
    if factor == -1.0:
        return -a
    return a * factor


def rotated(value, step, length, orient):
    step %= length
    quarter, rest = divmod(4 * step, length)
    real, imag = value
    if rest == 0:
        cosine = (1.0, 0.0, -1.0, 0.0)[quarter]
        sine = (0.0, 1.0, 0.0, -1.0)[quarter] * orient
    else:
        cosine = math.cos(2.0 * math.pi * step / length)
        sine = orient * math.sin(2.0 * math.pi * step / length)
    return (
        minus(scaled(real, cosine), scaled(imag, sine)),
        plus(scaled(real, sine), scaled(imag, cosine)),
    )


def transformed(values, orient):
    length = len(values)
    if length == 1:
        return values
    even = transformed(values[0::2], orient)
    odd = transformed(values[1::2], orient)
    front, rear = [], []
    for k in range(length // 2):
        turned = rotated(odd[k], k, length, orient)
        front.append((plus(even[k][0], turned[0]), plus(even[k][1], turned[1])))
        rear.append((minus(even[k][0], turned[0]), minus(even[k][1], turned[1])))
    return front + rear


def transformed_real(values):
    length = len(values)
    if length == 1:
        return [(values[0], None)]
    if length == 2:
        return [(values[0] + values[1], None), (values[0] - values[1], None)]
    even = transformed_real(values[0::2])
    odd = transformed_real(values[1::2])
    out = [None] * (length // 2 + 1)
    for k in range(length // 4 + 1):
        turned = rotated(odd[k], k, length, -1.0)
        out[k] = (plus(even[k][0], turned[0]), plus(even[k][1], turned[1]))
        mirror_imag = minus(turned[1], even[k][1])
        out[length // 2 - k] = (minus(even[k][0], turned[0]), mirror_imag)
    return out


def split(value):
    high = value.astype(BF16)
    return high, (value - high.astype(jnp.float32)).astype(BF16)


def product(left, right, dims=((1,), (0,))):
    return lax.dot_general(left, right, (dims, ((), ())), preferred_element_type=jnp.float32)


def table_times(table_ref, value):
    size = value.shape[0]
    high, low = split(value)
    stacked = jnp.concatenate([high, low, high], axis=0)
    left = jnp.concatenate([table_ref[:, :size], table_ref[:, :size], table_ref[:, size:]], axis=1)
    return product(left, stacked)


def table_times_rows(table_ref, value):
    size = value.shape[1]
    high, low = split(value)
    stacked = jnp.concatenate([high, low, high], axis=1)
    left = jnp.concatenate([table_ref[:, :size], table_ref[:, :size], table_ref[:, size:]], axis=1)
    return product(left, stacked, ((1,), (1,)))


def times_table(value, table_ref):
    size = value.shape[1]
    high, low = split(value)
    stacked = jnp.concatenate([high, low, high], axis=1)
    right = jnp.concatenate([table_ref[:size], table_ref[:size], table_ref[size:]], axis=0)
    return product(stacked, right)


def rows_forth_kernel(*refs):
    field_refs = refs[:6]
    turn_ref, forth_ref, out_ref, held_ref = refs[6:]
    for block in range(4):
        rows = slice(8 * block, 8 * block + 8)
        pieces = []
        for n in range(SHORT):
            terms, start = part_terms(field_refs, LONG * n)
            lanes = slice(LONG * n - start, LONG * n - start + LONG)
            total = terms[0][rows, lanes]
            for term in terms[1:]:
                total = total + term[rows, lanes]
            pieces.append(total)
        half = transformed_real(pieces)
        for k in range(SHORT):
            real, imag = half[k] if k <= SHORT // 2 else half[SHORT - k]
            if k > SHORT // 2:
                imag = None if imag is None else -imag
            cosine = turn_ref[0, k : k + 1, :]
            sine = turn_ref[1, k : k + 1, :]
            if imag is None:
                held_ref[k, block, :, :LONG] = real * cosine
                held_ref[k, block, :, LONG:] = -(real * sine)
            else:
                held_ref[k, block, :, :LONG] = real * cosine + imag * sine
                held_ref[k, block, :, LONG:] = imag * cosine - real * sine
    for quarter in range(4):
        rows = held_ref[8 * quarter : 8 * quarter + 8].reshape(256, 2 * LONG)
        spread = table_times_rows(forth_ref, rows)
        for part in range(2):
            for side in range(2):
                tile = 8 * part + 2 * quarter + side
                out_ref[pl.ds(tile, LONG, FORTH), :] = spread[
                    LONG * part : LONG * part + LONG, LONG * side : LONG * side + LONG
                ]


def part_terms(refs, column):
    if column < EARLY:
        return refs[:2], 0
    return refs[2:6], EARLY


def columns_kernel(
    first_ref,
    arrived_ref,
    bins_ref,
    turn_ref,
    forth_ref,
    back_ref,
    short_forth_ref,
    short_back_ref,
    out_ref,
    power_ref,
    bands_ref,
):
    lane = lax.broadcasted_iota(jnp.int32, (LONG, LONG), 1)
    row = lax.broadcasted_iota(jnp.int32, (LONG, LONG), 0)
    height = row + LONG * (lane % SHORT)
    height = ((height + N // 2) % N - N // 2).astype(jnp.float32)
    height_square = height * height
    first = first_ref[0]
    for pair in range(4):
        columns = []
        for side in range(2):
            group = 2 * pair + side
            columns.append(
                jnp.concatenate(
                    [
                        arrived_ref[pl.ds(group, LONG, FORTH), :],
                        arrived_ref[pl.ds(8 + group, LONG, FORTH), :],
                    ],
                    axis=0,
                )
            )
        spread = table_times(forth_ref, jnp.concatenate(columns, axis=1))
        cosine = turn_ref[0]
        sine = turn_ref[1]
        turned = []
        for side in range(2):
            lanes = slice(LONG * side, LONG * side + LONG)
            real, imag = spread[:LONG, lanes], spread[LONG:, lanes]
            turned.append(
                jnp.concatenate([real * cosine + imag * sine, imag * cosine - real * sine], axis=1)
            )
        held = times_table(jnp.concatenate(turned, axis=0), short_forth_ref)
        hats = []
        for side in range(2):
            group = 2 * pair + side
            real = held[LONG * side : LONG * side + LONG, :LONG]
            imag = held[LONG * side : LONG * side + LONG, LONG:]
            across = first + 4 * group + lane // SHORT
            across = ((across + N // 2) % N - N // 2).astype(jnp.float32)
            across_square = across * across
            square_norm = height_square + across_square
            anchor = square_norm == 0.0
            real = jnp.where(anchor, 0.0, real)
            imag = jnp.where(anchor, 0.0, imag)
            power_ref[LONG * group : LONG * group + LONG, :] = real * real + imag * imag
            inverse = (1.0 / float(N) ** 2) / jnp.where(anchor, 1.0, square_norm)
            kernel_real = (across_square - height_square) * inverse
            kernel_imag = (across * height) * (2.0 * inverse)
            hats.append(
                jnp.concatenate(
                    [
                        kernel_real * real - kernel_imag * imag,
                        kernel_real * imag + kernel_imag * real,
                    ],
                    axis=1,
                )
            )
        returned = times_table(jnp.concatenate(hats, axis=0), short_back_ref)
        columns = []
        for side in range(2):
            rows = slice(LONG * side, LONG * side + LONG)
            real, imag = returned[rows, :LONG], returned[rows, LONG:]
            columns.append(
                jnp.concatenate([real * cosine - imag * sine, imag * cosine + real * sine], axis=0)
            )
        restored = table_times(back_ref, jnp.concatenate(columns, axis=1))
        for part in range(2):
            for side in range(2):
                tile = 8 * part + 2 * pair + side
                out_ref[pl.ds(tile, LONG, BACK), :] = restored[
                    LONG * part : LONG * part + LONG, LONG * side : LONG * side + LONG
                ]

    def one_block(block, carry):
        start = pl.multiple_of(block * 64, 64)
        power = power_ref[pl.ds(start, 64), :]
        bins = bins_ref[pl.ds(start, 64), :]
        for band in range(NBINS):
            chosen = jnp.where(bins == band, power, 0.0)
            bands_ref[8 * band : 8 * band + 8, :] += jnp.sum(chosen.reshape(8, 8, LONG), axis=0)
        return carry

    bands_ref[...] = jnp.zeros_like(bands_ref)
    lax.fori_loop(0, 8 * LONG // 64, one_block, 0)
    sums = jnp.sum(bands_ref[...].reshape(NBINS, 8, LONG), axis=1)
    sums = jnp.concatenate([sums, jnp.zeros((LONG - NBINS, LONG), jnp.float32)], axis=0)
    line = jnp.sum(sums.T, axis=0, keepdims=True) * (NBINS / float(N) ** 4)
    out_ref[pl.ds(16, LONG, BACK), :] = jnp.broadcast_to(line, (LONG, LONG))


def rows_back_kernel(
    arrived_ref, turn_ref, table_ref, real_ref, imag_ref, spectrum_ref, held_ref
):
    for group in range(8):
        pair = jnp.concatenate(
            [
                arrived_ref[pl.ds(group, LONG, BACK), :].T,
                arrived_ref[pl.ds(8 + group, LONG, BACK), :].T,
            ],
            axis=1,
        )
        held_ref[LONG * group : LONG * group + LONG, :] = times_table(pair, table_ref)
    bands = jnp.sum(arrived_ref[pl.ds(16, LONG, BACK), :], axis=0, keepdims=True)
    spectrum_ref[...] = bands[:, :NBINS]
    for block in range(4):
        pieces = []
        for k in range(SHORT):
            rows = slice(SHORT * k + 8 * block, SHORT * k + 8 * block + 8)
            cosine = turn_ref[0, k : k + 1, :]
            sine = turn_ref[1, k : k + 1, :]
            real, imag = held_ref[rows, :LONG], held_ref[rows, LONG:]
            pieces.append((real * cosine - imag * sine, imag * cosine + real * sine))
        for n, (real, imag) in enumerate(transformed(pieces, 1.0)):
            real_ref[8 * block : 8 * block + 8, LONG * n : LONG * n + LONG] = real
            imag_ref[8 * block : 8 * block + 8, LONG * n : LONG * n + LONG] = imag


def call(kernel, outs, scratch, inputs, smem_first=False):
    whole = pl.BlockSpec(memory_space=pltpu.VMEM)
    specs = [whole] * len(inputs)
    if smem_first:
        specs[0] = pl.BlockSpec(memory_space=pltpu.SMEM)
    return pl.pallas_call(
        kernel,
        out_shape=outs,
        in_specs=specs,
        out_specs=jax.tree.map(lambda _: whole, outs),
        scratch_shapes=scratch,
        compiler_params=pltpu.CompilerParams(vmem_limit_bytes=48 * 1024 * 1024),
    )(*inputs)


def f32(*shape):
    return jax.ShapeDtypeStruct(shape, jnp.float32)


def exchanged(array, height):
    blocks = array.reshape(LONG, 1, height * LONG)
    blocks = lax.all_to_all(blocks, ROWS_PLANES, split_axis=0, concat_axis=0, tiled=True)
    return blocks.reshape(LONG * height, LONG)


def along(array, step):
    return lax.ppermute(array, PLANES[0], [(i, (i + step) % 4) for i in range(4)])


def swapped(array):
    return lax.ppermute(array, PLANES[1], [(0, 1), (1, 0)])


def apart(array):
    return lax.optimization_barrier(array)


def added_kernel(index_ref, scale_ref, own_ref, far_ref, out_ref):
    out_ref[...] = own_ref[0] * scale_ref[0] + far_ref[...]


def added(index, scale, whole, side, far):
    shape = (1,) + far.shape
    lead = (0,) * (len(shape) - 2)
    here = lambda i, index_ref: (index_ref[0],) + lead + (side,)
    rest = lambda i, index_ref: lead + (0,)
    grid_spec = pltpu.PrefetchScalarGridSpec(
        num_scalar_prefetch=1,
        grid=(1,),
        in_specs=[
            pl.BlockSpec(memory_space=pltpu.SMEM),
            pl.BlockSpec(shape, here),
            pl.BlockSpec(far.shape, rest),
        ],
        out_specs=pl.BlockSpec(far.shape, rest),
    )
    return pl.pallas_call(
        added_kernel, grid_spec=grid_spec, out_shape=f32(*far.shape), name="added"
    )(index.reshape(1), scale.reshape(1), whole, far)


def summed_along(piece, bound):
    far_up = along(piece(2, 0), 1)
    far_down = along(piece(2, 1), -1)
    up_free = along(piece(1, 1), 1)
    down_free = along(piece(-1, 0), -1)
    up_bound = along(bound(1, 0, far_up), 1)
    down_bound = along(bound(-1, 1, far_down), -1)
    return (up_bound, down_free), (up_free, down_bound)


def plane_sum(density, weight):
    length = density.shape[-1]
    here = lax.axis_index(PLANES[0])
    upper = lax.axis_index(PLANES[1])
    blocks = density.reshape(4, 2, -1, length)
    rows = blocks.shape[2]

    def early(step, side):
        got = lax.dynamic_slice(
            blocks, ((here + step) & 3, 0, 0, side * EARLY_HALF), (1, 2, rows, EARLY_HALF)
        )
        return got[0] * weight

    def early_bound(step, side, far):
        return added((here + step) & 3, weight, blocks, side, far)

    def late_block(half):
        got = lax.dynamic_slice(
            blocks, (0, half, 0, EARLY), (4, 1, rows, length - EARLY)
        )
        return got[:, 0] * weight

    late_other = swapped(late_block(1 - upper))
    left, right = summed_along(early, early_bound)
    late = apart(late_block(upper) + late_other)

    def late_piece(step):
        return lax.dynamic_index_in_dim(late, (here + step) & 3, 0, keepdims=False)

    early_sum = jnp.concatenate(
        [early(0, 0) + left[0] + left[1], early(0, 1) + right[0] + right[1]], axis=-1
    )
    mine = lax.dynamic_index_in_dim(early_sum, upper, 0, keepdims=False)
    other = swapped(lax.dynamic_index_in_dim(early_sum, 1 - upper, 0, keepdims=False))
    late_terms = [along(late_piece(step), step) for step in (1, -1, 2)]
    return (mine, other, late_piece(0), *late_terms)


def on_device(density, lens_weight, spectrum_bin):
    held = tables()
    device = lax.axis_index(ROWS_PLANES)
    parts = plane_sum(density[0], lens_weight[0])
    bins = spectrum_bin.reshape(SHORT, LONG, 8, 4).transpose(2, 1, 3, 0).reshape(8 * LONG, LONG)
    sent = call(
        rows_forth_kernel,
        f32(LONG * FORTH, LONG),
        [pltpu.VMEM((SHORT, 4, 8, 2 * LONG), jnp.float32)],
        (*parts, held["row_turn"], held["forth"]),
    )
    arrived = exchanged(sent, FORTH)
    sent = call(
        columns_kernel,
        f32(LONG * BACK, LONG),
        [pltpu.VMEM((8 * LONG, LONG), jnp.float32), pltpu.VMEM((8 * NBINS, LONG), jnp.float32)],
        (
            (device * SHORT).reshape(1),
            arrived,
            bins,
            held["column_turn"],
            held["forth"],
            held["back"],
            held["short_forth"],
            held["short_back"],
        ),
        smem_first=True,
    )
    arrived = exchanged(sent, BACK)
    shear_real, shear_imag, spectrum = call(
        rows_back_kernel,
        (f32(SHORT, N), f32(SHORT, N), f32(1, NBINS)),
        [pltpu.VMEM((8 * LONG, 2 * LONG), jnp.float32)],
        (arrived, held["row_turn"], held["right_back"]),
    )
    return shear_real, shear_imag, spectrum[0]


def solution(mesh):
    finer = Mesh(mesh.devices.reshape(4, 2, 2, 4, 2), ROWS_PLANES)
    in_specs = (P(PLANES, ROWS, None), P(PLANES), P(None, ROWS_PLANES))
    out_specs = (P(ROWS_PLANES, None), P(ROWS_PLANES, None), P())
    return jax.shard_map(
        on_device, mesh=finer, in_specs=in_specs, out_specs=out_specs, check_vma=False
    )
```

```python
import math

import numpy as np
import jax
import jax.numpy as jnp
from jax import lax
from jax.experimental import pallas as pl
from jax.experimental.pallas import tpu as pltpu
from jax.sharding import Mesh
from jax.sharding import PartitionSpec as P


N = 4096
LONG = 128
SHORT = 32
NBINS = 64
ROWS = ("rows_0", "rows_1", "rows_2")
PLANES = ("planes_0", "planes_1")
ROWS_PLANES = ROWS + PLANES
FORTH = 9
BACK = 17
EARLY_HALF = 1280
EARLY = 2 * EARLY_HALF
BF16 = jnp.bfloat16


def halves(table):
    high = table.astype(np.float32).astype(jnp.bfloat16)
    low = (table - high.astype(np.float64)).astype(np.float32).astype(jnp.bfloat16)
    return high, low


def tables():
    def wave(left, right, length):
        angle = 2.0 * np.pi * ((left[:, None] * right[None, :]) % length) / length
        return np.cos(angle), np.sin(angle)

    long_index = np.arange(LONG)
    short_index = np.arange(SHORT)
    cos_long, sin_long = wave(long_index, long_index, LONG)
    forth = np.block([[cos_long, sin_long], [-sin_long, cos_long]])
    cos_short, sin_short = wave(short_index, short_index, SHORT)
    cos_four, sin_four = np.kron(np.eye(4), cos_short), np.kron(np.eye(4), sin_short)
    short_forth = np.block([[cos_four, -sin_four], [sin_four, cos_four]])
    row_turn = wave(short_index, long_index, N)
    cos_turn, sin_turn = wave(long_index, short_index, N)
    column_turn = (np.tile(cos_turn, (1, 4)), np.tile(sin_turn, (1, 4)))
    return {
        "forth": np.concatenate(halves(forth), axis=1),
        "back": np.concatenate(halves(forth.T), axis=1),
        "short_forth": np.concatenate(halves(short_forth), axis=0),
        "short_back": np.concatenate(halves(short_forth.T), axis=0),
        "right_back": np.concatenate(halves(forth), axis=0),
        "row_turn": np.stack(row_turn).astype(np.float32),
        "column_turn": np.stack(column_turn).astype(np.float32),
    }


def plus(a, b):
    if a is None:
        return b
    if b is None:
        return a
    return a + b


def minus(a, b):
    if b is None:
        return a
    if a is None:
        return -b
    return a - b


def scaled(a, factor):
    if a is None or factor == 0.0:
        return None
    if factor == 1.0:
        return a
    if factor == -1.0:
        return -a
    return a * factor


def rotated(value, step, length, orient):
    step %= length
    quarter, rest = divmod(4 * step, length)
    real, imag = value
    if rest == 0:
        cosine = (1.0, 0.0, -1.0, 0.0)[quarter]
        sine = (0.0, 1.0, 0.0, -1.0)[quarter] * orient
    else:
        cosine = math.cos(2.0 * math.pi * step / length)
        sine = orient * math.sin(2.0 * math.pi * step / length)
    return (
        minus(scaled(real, cosine), scaled(imag, sine)),
        plus(scaled(real, sine), scaled(imag, cosine)),
    )


def transformed(values, orient):
    length = len(values)
    if length == 1:
        return values
    even = transformed(values[0::2], orient)
    odd = transformed(values[1::2], orient)
    front, rear = [], []
    for k in range(length // 2):
        turned = rotated(odd[k], k, length, orient)
        front.append((plus(even[k][0], turned[0]), plus(even[k][1], turned[1])))
        rear.append((minus(even[k][0], turned[0]), minus(even[k][1], turned[1])))
    return front + rear


def transformed_real(values):
    length = len(values)
    if length == 1:
        return [(values[0], None)]
    if length == 2:
        return [(values[0] + values[1], None), (values[0] - values[1], None)]
    even = transformed_real(values[0::2])
    odd = transformed_real(values[1::2])
    out = [None] * (length // 2 + 1)
    for k in range(length // 4 + 1):
        turned = rotated(odd[k], k, length, -1.0)
        out[k] = (plus(even[k][0], turned[0]), plus(even[k][1], turned[1]))
        mirror_imag = minus(turned[1], even[k][1])
        out[length // 2 - k] = (minus(even[k][0], turned[0]), mirror_imag)
    return out


def split(value):
    high = value.astype(BF16)
    return high, (value - high.astype(jnp.float32)).astype(BF16)


def product(left, right, dims=((1,), (0,))):
    return lax.dot_general(left, right, (dims, ((), ())), preferred_element_type=jnp.float32)


def table_times(table_ref, value):
    size = value.shape[0]
    high, low = split(value)
    stacked = jnp.concatenate([high, low, high], axis=0)
    left = jnp.concatenate([table_ref[:, :size], table_ref[:, :size], table_ref[:, size:]], axis=1)
    return product(left, stacked)


def table_times_rows(table_ref, value):
    size = value.shape[1]
    high, low = split(value)
    stacked = jnp.concatenate([high, low, high], axis=1)
    left = jnp.concatenate([table_ref[:, :size], table_ref[:, :size], table_ref[:, size:]], axis=1)
    return product(left, stacked, ((1,), (1,)))


def times_table(value, table_ref):
    size = value.shape[1]
    high, low = split(value)
    stacked = jnp.concatenate([high, low, high], axis=1)
    right = jnp.concatenate([table_ref[:size], table_ref[:size], table_ref[size:]], axis=0)
    return product(stacked, right)


def rows_forth_kernel(*refs):
    field_refs = refs[:6]
    turn_ref, forth_ref, out_ref, held_ref = refs[6:]
    for block in range(4):
        rows = slice(8 * block, 8 * block + 8)
        pieces = []
        for n in range(SHORT):
            terms, start = part_terms(field_refs, LONG * n)
            lanes = slice(LONG * n - start, LONG * n - start + LONG)
            total = terms[0][rows, lanes]
            for term in terms[1:]:
                total = total + term[rows, lanes]
            pieces.append(total)
        for k, (real, imag) in enumerate(transformed_real(pieces)):
            cosine = turn_ref[0, k : k + 1, :]
            sine = turn_ref[1, k : k + 1, :]
            if imag is None:
                held_ref[k, block, :, :LONG] = real * cosine
                held_ref[k, block, :, LONG:] = -(real * sine)
            else:
                held_ref[k, block, :, :LONG] = real * cosine + imag * sine
                held_ref[k, block, :, LONG:] = imag * cosine - real * sine
    for half in range(2):
        rows = held_ref[8 * half : 8 * half + 8].reshape(256, 2 * LONG)
        spread = table_times_rows(forth_ref, rows)
        for part in range(2):
            for side in range(2):
                tile = 4 * part + 2 * half + side
                out_ref[pl.ds(tile, LONG, FORTH), :] = spread[
                    LONG * part : LONG * part + LONG, LONG * side : LONG * side + LONG
                ]
    last = held_ref[SHORT // 2].reshape(SHORT, 2 * LONG)
    real, imag = last[:, :LONG], last[:, LONG:]
    turned = jnp.concatenate([imag, -real], axis=1)
    nothing = jnp.zeros((2 * SHORT, 2 * LONG), jnp.float32)
    spread = table_times_rows(forth_ref, jnp.concatenate([last, turned, nothing], axis=0))
    out_ref[pl.ds(8, LONG, FORTH), :] = spread[:LONG]


def part_terms(refs, column):
    if column < EARLY:
        return refs[:2], 0
    return refs[2:6], EARLY


def columns_kernel(
    first_ref,
    arrived_ref,
    bins_ref,
    mirror_ref,
    middle_ref,
    turn_ref,
    forth_ref,
    back_ref,
    short_forth_ref,
    short_back_ref,
    out_ref,
    power_ref,
    bands_ref,
):
    lane = lax.broadcasted_iota(jnp.int32, (LONG, LONG), 1)
    row = lax.broadcasted_iota(jnp.int32, (LONG, LONG), 0)
    height = row + LONG * (lane % SHORT)
    height = ((height + N // 2) % N - N // 2).astype(jnp.float32)
    height_square = height * height
    first = first_ref[0]
    cosine = turn_ref[0]
    sine = turn_ref[1]
    lone = lane < SHORT
    edge = height == -(N // 2)

    def forth(tiles):
        spread = table_times(
            forth_ref, jnp.concatenate([jnp.concatenate(tile, axis=0) for tile in tiles], axis=1)
        )
        turned = []
        for side in range(len(tiles)):
            lanes = slice(LONG * side, LONG * side + LONG)
            real, imag = spread[:LONG, lanes], spread[LONG:, lanes]
            turned.append(
                jnp.concatenate([real * cosine + imag * sine, imag * cosine - real * sine], axis=1)
            )
        held = times_table(jnp.concatenate(turned, axis=0), short_forth_ref)
        rows = [slice(LONG * side, LONG * side + LONG) for side in range(len(tiles))]
        return [(held[r, :LONG], held[r, LONG:]) for r in rows]

    def kernels(group, pair):
        real, imag = pair
        across = first + 4 * group + lane // SHORT
        across = ((across + N // 2) % N - N // 2).astype(jnp.float32)
        across_square = across * across
        square_norm = height_square + across_square
        anchor = square_norm == 0.0
        real = jnp.where(anchor, 0.0, real)
        imag = jnp.where(anchor, 0.0, imag)
        inverse = (1.0 / float(N) ** 2) / jnp.where(anchor, 1.0, square_norm)
        kernel_real = (across_square - height_square) * inverse
        kernel_imag = (across * height) * (2.0 * inverse)
        return real, imag, kernel_real, kernel_imag

    def back(hats):
        returned = times_table(jnp.concatenate(hats, axis=0), short_back_ref)
        columns = []
        for side in range(2):
            rows = slice(LONG * side, LONG * side + LONG)
            real, imag = returned[rows, :LONG], returned[rows, LONG:]
            columns.append(
                jnp.concatenate([real * cosine - imag * sine, imag * cosine + real * sine], axis=0)
            )
        return table_times(back_ref, jnp.concatenate(columns, axis=1))

    middle = arrived_ref[pl.ds(8, LONG, FORTH), :]
    tile = (jnp.where(lone, middle, 0.0), jnp.where(lone, pltpu.roll(middle, 96, 1), 0.0))
    real, imag, kernel_real, kernel_imag = kernels(4, forth([tile])[0])
    middle_power = real * real + imag * imag
    middle_hat = (kernel_real * real - kernel_imag * imag, kernel_real * imag + kernel_imag * real)
    for pair in range(2):
        tiles = [
            (arrived_ref[pl.ds(g, LONG, FORTH), :], arrived_ref[pl.ds(4 + g, LONG, FORTH), :])
            for g in (2 * pair, 2 * pair + 1)
        ]
        hats_a, hats_b = [], []
        for side, got in enumerate(forth(tiles)):
            group = 2 * pair + side
            real, imag, kernel_real, kernel_imag = kernels(group, got)
            power = real * real + imag * imag
            single = edge | lone if group == 0 else edge
            odd = jnp.where(single, kernel_imag, 0.0)
            even = jnp.where(single, 0.0, kernel_imag)
            b_real, b_imag = even * real, even * imag
            mirror_power = power
            if group == 0:
                b_real = jnp.where(lone, middle_hat[0], b_real)
                b_imag = jnp.where(lone, middle_hat[1], b_imag)
                mirror_power = jnp.where(lone, middle_power, power)
            power_ref[LONG * group : LONG * group + LONG, :] = power
            power_ref[LONG * (4 + group) : LONG * (5 + group), :] = mirror_power
            hats_a.append(
                jnp.concatenate(
                    [kernel_real * real - odd * imag, kernel_real * imag + odd * real], axis=1
                )
            )
            hats_b.append(jnp.concatenate([b_real, b_imag], axis=1))
        for which, hats in enumerate((hats_a, hats_b)):
            restored = back(hats)
            for part in range(2):
                for side in range(2):
                    tile = 8 * part + 4 * which + 2 * pair + side
                    out_ref[pl.ds(tile, LONG, BACK), :] = restored[
                        LONG * part : LONG * part + LONG, LONG * side : LONG * side + LONG
                    ]

    def counted(tile_ref, offset, inner=None):
        def one_block(block, carry):
            start = pl.multiple_of(block * 64, 64)
            power = power_ref[pl.ds(offset + start, 64), :]
            bins = tile_ref[pl.ds(start, 64), :]
            if inner is not None:
                row = jnp.minimum(start, LONG - 64)
                here = (lane[:64] < SHORT) & (start < LONG)
                bins = jnp.where(here, inner[pl.ds(pl.multiple_of(row, 64), 64), :], bins)
            for band in range(NBINS):
                chosen = jnp.where(bins == band, power, 0.0)
                bands_ref[8 * band : 8 * band + 8, :] += jnp.sum(
                    chosen.reshape(8, 8, LONG), axis=0
                )
            return carry

        lax.fori_loop(0, 4 * LONG // 64, one_block, 0)

    bands_ref[...] = jnp.zeros_like(bands_ref)
    counted(bins_ref, 0)
    counted(mirror_ref, 4 * LONG, middle_ref)
    sums = jnp.sum(bands_ref[...].reshape(NBINS, 8, LONG), axis=1)
    sums = jnp.concatenate([sums, jnp.zeros((LONG - NBINS, LONG), jnp.float32)], axis=0)
    line = jnp.sum(sums.T, axis=0, keepdims=True) * (NBINS / float(N) ** 4)
    out_ref[pl.ds(16, LONG, BACK), :] = jnp.broadcast_to(line, (LONG, LONG))


def rows_back_kernel(
    arrived_ref, turn_ref, table_ref, real_ref, imag_ref, spectrum_ref, held_ref
):
    for group in range(8):
        pair = jnp.concatenate(
            [
                arrived_ref[pl.ds(group, LONG, BACK), :].T,
                arrived_ref[pl.ds(8 + group, LONG, BACK), :].T,
            ],
            axis=1,
        )
        held_ref[LONG * group : LONG * group + LONG, :] = times_table(pair, table_ref)
    bands = jnp.sum(arrived_ref[pl.ds(16, LONG, BACK), :], axis=0, keepdims=True)
    spectrum_ref[...] = bands[:, :NBINS]
    for block in range(4):
        pieces = [None] * SHORT
        for k in range(SHORT // 2):
            turned = []
            for which in range(2):
                start = SHORT * (SHORT // 2 * which + k) + 8 * block
                rows = slice(start, start + 8)
                turn = k + SHORT // 2 if which and not k else k
                cosine = turn_ref[0, turn : turn + 1, :]
                sine = turn_ref[1, turn : turn + 1, :]
                real, imag = held_ref[rows, :LONG], held_ref[rows, LONG:]
                turned.append((real * cosine - imag * sine, imag * cosine + real * sine))
            (a_real, a_imag), (b_real, b_imag) = turned
            if k == 0:
                pieces[0], pieces[SHORT // 2] = turned
            else:
                pieces[k] = (a_real - b_imag, a_imag + b_real)
                pieces[SHORT - k] = (a_real + b_imag, b_real - a_imag)
        for n, (real, imag) in enumerate(transformed(pieces, 1.0)):
            real_ref[8 * block : 8 * block + 8, LONG * n : LONG * n + LONG] = real
            imag_ref[8 * block : 8 * block + 8, LONG * n : LONG * n + LONG] = imag


def call(kernel, outs, scratch, inputs, smem_first=False):
    whole = pl.BlockSpec(memory_space=pltpu.VMEM)
    specs = [whole] * len(inputs)
    if smem_first:
        specs[0] = pl.BlockSpec(memory_space=pltpu.SMEM)
    return pl.pallas_call(
        kernel,
        out_shape=outs,
        in_specs=specs,
        out_specs=jax.tree.map(lambda _: whole, outs),
        scratch_shapes=scratch,
        compiler_params=pltpu.CompilerParams(vmem_limit_bytes=48 * 1024 * 1024),
    )(*inputs)


def f32(*shape):
    return jax.ShapeDtypeStruct(shape, jnp.float32)


def exchanged(array, height):
    blocks = array.reshape(LONG, 1, height * LONG)
    blocks = lax.all_to_all(blocks, ROWS_PLANES, split_axis=0, concat_axis=0, tiled=True)
    return blocks.reshape(LONG * height, LONG)


def along(array, step):
    return lax.ppermute(array, PLANES[0], [(i, (i + step) % 4) for i in range(4)])


def swapped(array):
    return lax.ppermute(array, PLANES[1], [(0, 1), (1, 0)])


def after(array, other):
    return lax.optimization_barrier((array, other))[0]


def plane_sum(density, weight):
    length = density.shape[-1]
    here = lax.axis_index(PLANES[0])
    upper = lax.axis_index(PLANES[1])
    blocks = density.reshape(4, 2, -1, length)
    rows = blocks.shape[2]

    def early(source, step, side):
        got = lax.dynamic_slice(
            source, ((here + step) & 3, 0, 0, side * EARLY_HALF), (1, 2, rows, EARLY_HALF)
        )
        return got[0] * weight

    def late_block(source, half):
        got = lax.dynamic_slice(source, (0, half, 0, EARLY), (4, 1, rows, length - EARLY))
        return got[:, 0] * weight

    far_up = along(early(blocks, 2, 0), 1)
    far_down = along(early(blocks, 2, 1), -1)
    late_sent = late_block(blocks, 1 - upper)
    late_other = swapped(late_sent)
    up_free = along(early(blocks, 1, 1), 1)
    down_free = along(early(blocks, -1, 0), -1)
    up_bound = along(early(after(blocks, far_up), 1, 0) + far_up, 1)
    down_bound = along(early(after(blocks, far_down), -1, 1) + far_down, -1)
    late = late_block(after(blocks, late_other), upper) + late_other

    def late_piece(step):
        return lax.dynamic_index_in_dim(late, (here + step) & 3, 0, keepdims=False)

    late_terms = [along(late_piece(step), step) for step in (1, -1, 2)]
    whole = after(blocks, up_bound)
    early_sum = jnp.concatenate(
        [
            early(whole, 0, 0) + up_bound + down_free,
            early(whole, 0, 1) + up_free + down_bound,
        ],
        axis=-1,
    )
    sent = lax.dynamic_index_in_dim(early_sum, 1 - upper, 0, keepdims=False)
    mine = lax.dynamic_index_in_dim(early_sum, upper, 0, keepdims=False)
    other = swapped(sent)
    return (mine, other, late_piece(0), *late_terms)


def tiled(columns):
    return columns.reshape(4, 4, SHORT, LONG).transpose(0, 3, 1, 2).reshape(4 * LONG, LONG)


def swapped_mirror(array):
    return lax.ppermute(array, ROWS_PLANES, [(i, LONG - 1 - i) for i in range(LONG)])


def on_device(density, lens_weight, spectrum_bin):
    held = tables()
    device = lax.axis_index(ROWS_PLANES)
    parts = plane_sum(density[0], lens_weight[0])
    columns = spectrum_bin.T
    mirrored = jnp.roll(columns[SHORT // 2 + 1 :, ::-1], 1, axis=1)[::-1]
    mirrored = tiled(jnp.concatenate([columns[:1], mirrored], axis=0))
    bins = tiled(columns[: SHORT // 2])
    middle = columns[SHORT // 2].reshape(SHORT, LONG).T
    middle = jnp.pad(middle, ((0, 0), (0, 3 * SHORT)))
    mirror = swapped_mirror(after(mirrored, parts[1]))
    sent = call(
        rows_forth_kernel,
        f32(LONG * FORTH, LONG),
        [pltpu.VMEM((SHORT, 4, 8, 2 * LONG), jnp.float32)],
        (*parts, held["row_turn"], held["forth"]),
    )
    arrived = exchanged(sent, FORTH)
    sent = call(
        columns_kernel,
        f32(LONG * BACK, LONG),
        [pltpu.VMEM((8 * LONG, LONG), jnp.float32), pltpu.VMEM((8 * NBINS, LONG), jnp.float32)],
        (
            (device * SHORT).reshape(1),
            arrived,
            bins,
            mirror,
            middle,
            held["column_turn"],
            held["forth"],
            held["back"],
            held["short_forth"],
            held["short_back"],
        ),
        smem_first=True,
    )
    arrived = exchanged(sent, BACK)
    shear_real, shear_imag, spectrum = call(
        rows_back_kernel,
        (f32(SHORT, N), f32(SHORT, N), f32(1, NBINS)),
        [pltpu.VMEM((8 * LONG, 2 * LONG), jnp.float32)],
        (arrived, held["row_turn"], held["right_back"]),
    )
    return shear_real, shear_imag, spectrum[0]


def solution(mesh):
    finer = Mesh(mesh.devices.reshape(4, 2, 2, 4, 2), ROWS_PLANES)
    in_specs = (P(PLANES, ROWS, None), P(PLANES), P(None, ROWS_PLANES))
    out_specs = (P(ROWS_PLANES, None), P(ROWS_PLANES, None), P())
    return jax.shard_map(
        on_device, mesh=finer, in_specs=in_specs, out_specs=out_specs, check_vma=False
    )
```

```python
import math

import numpy as np
import jax
import jax.numpy as jnp
from jax import lax
from jax.experimental import pallas as pl
from jax.experimental.pallas import tpu as pltpu
from jax.sharding import Mesh
from jax.sharding import PartitionSpec as P


N = 4096
LONG = 128
SHORT = 32
NBINS = 64
ROWS = ("rows_0", "rows_1", "rows_2")
PLANES = ("planes_0", "planes_1")
ROWS_PLANES = ROWS + PLANES
FORTH = 9
BACK = 17
EARLY_HALF = 1280
EARLY = 2 * EARLY_HALF
BF16 = jnp.bfloat16


def halves(table):
    high = table.astype(np.float32).astype(jnp.bfloat16)
    low = (table - high.astype(np.float64)).astype(np.float32).astype(jnp.bfloat16)
    return high, low


def tables():
    def wave(left, right, length):
        angle = 2.0 * np.pi * ((left[:, None] * right[None, :]) % length) / length
        return np.cos(angle), np.sin(angle)

    long_index = np.arange(LONG)
    short_index = np.arange(SHORT)
    cos_long, sin_long = wave(long_index, long_index, LONG)
    forth = np.block([[cos_long, sin_long], [-sin_long, cos_long]])
    cos_short, sin_short = wave(short_index, short_index, SHORT)
    cos_four, sin_four = np.kron(np.eye(4), cos_short), np.kron(np.eye(4), sin_short)
    short_forth = np.block([[cos_four, -sin_four], [sin_four, cos_four]])
    row_turn = wave(short_index, long_index, N)
    cos_turn, sin_turn = wave(long_index, short_index, N)
    column_turn = (np.tile(cos_turn, (1, 4)), np.tile(sin_turn, (1, 4)))
    return {
        "forth": np.concatenate(halves(forth), axis=1),
        "back": np.concatenate(halves(forth.T), axis=1),
        "short_forth": np.concatenate(halves(short_forth), axis=0),
        "short_back": np.concatenate(halves(short_forth.T), axis=0),
        "right_back": np.concatenate(halves(forth), axis=0),
        "row_turn": np.stack(row_turn).astype(np.float32),
        "column_turn": np.stack(column_turn).astype(np.float32),
    }


def plus(a, b):
    if a is None:
        return b
    if b is None:
        return a
    return a + b


def minus(a, b):
    if b is None:
        return a
    if a is None:
        return -b
    return a - b


def scaled(a, factor):
    if a is None or factor == 0.0:
        return None
    if factor == 1.0:
        return a
    if factor == -1.0:
        return -a
    return a * factor


def rotated(value, step, length, orient):
    step %= length
    quarter, rest = divmod(4 * step, length)
    real, imag = value
    if rest == 0:
        cosine = (1.0, 0.0, -1.0, 0.0)[quarter]
        sine = (0.0, 1.0, 0.0, -1.0)[quarter] * orient
    else:
        cosine = math.cos(2.0 * math.pi * step / length)
        sine = orient * math.sin(2.0 * math.pi * step / length)
    return (
        minus(scaled(real, cosine), scaled(imag, sine)),
        plus(scaled(real, sine), scaled(imag, cosine)),
    )


def transformed(values, orient):
    length = len(values)
    if length == 1:
        return values
    even = transformed(values[0::2], orient)
    odd = transformed(values[1::2], orient)
    front, rear = [], []
    for k in range(length // 2):
        turned = rotated(odd[k], k, length, orient)
        front.append((plus(even[k][0], turned[0]), plus(even[k][1], turned[1])))
        rear.append((minus(even[k][0], turned[0]), minus(even[k][1], turned[1])))
    return front + rear


def transformed_real(values):
    length = len(values)
    if length == 1:
        return [(values[0], None)]
    if length == 2:
        return [(values[0] + values[1], None), (values[0] - values[1], None)]
    even = transformed_real(values[0::2])
    odd = transformed_real(values[1::2])
    out = [None] * (length // 2 + 1)
    for k in range(length // 4 + 1):
        turned = rotated(odd[k], k, length, -1.0)
        out[k] = (plus(even[k][0], turned[0]), plus(even[k][1], turned[1]))
        mirror_imag = minus(turned[1], even[k][1])
        out[length // 2 - k] = (minus(even[k][0], turned[0]), mirror_imag)
    return out


def split(value):
    high = value.astype(BF16)
    return high, (value - high.astype(jnp.float32)).astype(BF16)


def product(left, right, dims=((1,), (0,))):
    return lax.dot_general(left, right, (dims, ((), ())), preferred_element_type=jnp.float32)


def table_times(table_ref, value):
    size = value.shape[0]
    high, low = split(value)
    stacked = jnp.concatenate([high, low, high], axis=0)
    left = jnp.concatenate([table_ref[:, :size], table_ref[:, :size], table_ref[:, size:]], axis=1)
    return product(left, stacked)


def table_times_rows(table_ref, value):
    size = value.shape[1]
    high, low = split(value)
    stacked = jnp.concatenate([high, low, high], axis=1)
    left = jnp.concatenate([table_ref[:, :size], table_ref[:, :size], table_ref[:, size:]], axis=1)
    return product(left, stacked, ((1,), (1,)))


def times_table(value, table_ref):
    size = value.shape[1]
    high, low = split(value)
    stacked = jnp.concatenate([high, low, high], axis=1)
    right = jnp.concatenate([table_ref[:size], table_ref[:size], table_ref[size:]], axis=0)
    return product(stacked, right)


def rows_forth_kernel(*refs):
    field_refs = refs[:6]
    turn_ref, forth_ref, out_ref, held_ref = refs[6:]
    for block in range(4):
        rows = slice(8 * block, 8 * block + 8)
        pieces = []
        for n in range(SHORT):
            terms, start = part_terms(field_refs, LONG * n)
            lanes = slice(LONG * n - start, LONG * n - start + LONG)
            total = terms[0][rows, lanes]
            for term in terms[1:]:
                total = total + term[rows, lanes]
            pieces.append(total)
        for k, (real, imag) in enumerate(transformed_real(pieces)):
            cosine = turn_ref[0, k : k + 1, :]
            sine = turn_ref[1, k : k + 1, :]
            if imag is None:
                held_ref[k, block, :, :LONG] = real * cosine
                held_ref[k, block, :, LONG:] = -(real * sine)
            else:
                held_ref[k, block, :, :LONG] = real * cosine + imag * sine
                held_ref[k, block, :, LONG:] = imag * cosine - real * sine
    for half in range(2):
        rows = held_ref[8 * half : 8 * half + 8].reshape(256, 2 * LONG)
        spread = table_times_rows(forth_ref, rows)
        for part in range(2):
            for side in range(2):
                tile = 4 * part + 2 * half + side
                out_ref[pl.ds(tile, LONG, FORTH), :] = spread[
                    LONG * part : LONG * part + LONG, LONG * side : LONG * side + LONG
                ]
    last = held_ref[SHORT // 2].reshape(SHORT, 2 * LONG)
    real, imag = last[:, :LONG], last[:, LONG:]
    turned = jnp.concatenate([imag, -real], axis=1)
    nothing = jnp.zeros((2 * SHORT, 2 * LONG), jnp.float32)
    spread = table_times_rows(forth_ref, jnp.concatenate([last, turned, nothing], axis=0))
    out_ref[pl.ds(8, LONG, FORTH), :] = spread[:LONG]


def part_terms(refs, column):
    if column < EARLY:
        return refs[:2], 0
    return refs[2:6], EARLY


def columns_kernel(
    first_ref,
    arrived_ref,
    bins_ref,
    mirror_ref,
    middle_ref,
    turn_ref,
    forth_ref,
    back_ref,
    short_forth_ref,
    short_back_ref,
    out_ref,
    bands_ref,
):
    lane = lax.broadcasted_iota(jnp.int32, (LONG, LONG), 1)
    row = lax.broadcasted_iota(jnp.int32, (LONG, LONG), 0)
    height = row + LONG * (lane % SHORT)
    height = ((height + N // 2) % N - N // 2).astype(jnp.float32)
    height_square = height * height
    first = first_ref[0]
    cosine = turn_ref[0]
    sine = turn_ref[1]
    lone = lane < SHORT
    edge = height == -(N // 2)

    def forth(tiles):
        spread = table_times(
            forth_ref, jnp.concatenate([jnp.concatenate(tile, axis=0) for tile in tiles], axis=1)
        )
        turned = []
        for side in range(len(tiles)):
            lanes = slice(LONG * side, LONG * side + LONG)
            real, imag = spread[:LONG, lanes], spread[LONG:, lanes]
            turned.append(
                jnp.concatenate([real * cosine + imag * sine, imag * cosine - real * sine], axis=1)
            )
        held = times_table(jnp.concatenate(turned, axis=0), short_forth_ref)
        rows = [slice(LONG * side, LONG * side + LONG) for side in range(len(tiles))]
        return [(held[r, :LONG], held[r, LONG:]) for r in rows]

    def kernels(group, pair):
        real, imag = pair
        across = first + 4 * group + lane // SHORT
        across = ((across + N // 2) % N - N // 2).astype(jnp.float32)
        across_square = across * across
        square_norm = height_square + across_square
        anchor = square_norm == 0.0
        real = jnp.where(anchor, 0.0, real)
        imag = jnp.where(anchor, 0.0, imag)
        inverse = (1.0 / float(N) ** 2) / jnp.where(anchor, 1.0, square_norm)
        kernel_real = (across_square - height_square) * inverse
        kernel_imag = (across * height) * (2.0 * inverse)
        return real, imag, kernel_real, kernel_imag

    def back(hats):
        returned = times_table(jnp.concatenate(hats, axis=0), short_back_ref)
        columns = []
        for side in range(2):
            rows = slice(LONG * side, LONG * side + LONG)
            real, imag = returned[rows, :LONG], returned[rows, LONG:]
            columns.append(
                jnp.concatenate([real * cosine - imag * sine, imag * cosine + real * sine], axis=0)
            )
        return table_times(back_ref, jnp.concatenate(columns, axis=1))

    bands_ref[...] = jnp.zeros_like(bands_ref)

    def counted(group, power, mirror_power):
        rows = slice(LONG * group, LONG * group + LONG)
        mirror_bins = mirror_ref[rows]
        if group == 0:
            mirror_bins = jnp.where(lone, middle_ref[...], mirror_bins)
        for got, bins in ((power, bins_ref[rows]), (mirror_power, mirror_bins)):
            high = got.astype(BF16).astype(jnp.float32)
            low = got - high
            coarse, fine = bins >> 3, bins & 7
            values, marks = [], []
            for start in range(0, LONG, 8):
                here = slice(start, start + 8)
                chosen = [coarse[here] == index for index in range(8)]
                stack = [jnp.where(mask, high[here], 0.0) for mask in chosen]
                stack += [jnp.where(mask, low[here], 0.0) for mask in chosen]
                values.append(jnp.concatenate(stack, axis=0).astype(BF16))
                stack = [jnp.where(fine[here] == index, 1.0, 0.0) for index in range(8)]
                marks.append(jnp.concatenate(stack, axis=0).astype(BF16))
            bands_ref[...] += product(
                jnp.concatenate(values, axis=1), jnp.concatenate(marks, axis=1), ((1,), (1,))
            )

    middle = arrived_ref[pl.ds(8, LONG, FORTH), :]
    tile = (jnp.where(lone, middle, 0.0), jnp.where(lone, pltpu.roll(middle, 96, 1), 0.0))
    real, imag, kernel_real, kernel_imag = kernels(4, forth([tile])[0])
    middle_power = real * real + imag * imag
    middle_hat = (kernel_real * real - kernel_imag * imag, kernel_real * imag + kernel_imag * real)
    for pair in range(2):
        tiles = [
            (arrived_ref[pl.ds(g, LONG, FORTH), :], arrived_ref[pl.ds(4 + g, LONG, FORTH), :])
            for g in (2 * pair, 2 * pair + 1)
        ]
        hats_a, hats_b = [], []
        for side, got in enumerate(forth(tiles)):
            group = 2 * pair + side
            real, imag, kernel_real, kernel_imag = kernels(group, got)
            power = real * real + imag * imag
            single = edge | lone if group == 0 else edge
            odd = jnp.where(single, kernel_imag, 0.0)
            even = jnp.where(single, 0.0, kernel_imag)
            b_real, b_imag = even * real, even * imag
            mirror_power = power
            if group == 0:
                b_real = jnp.where(lone, middle_hat[0], b_real)
                b_imag = jnp.where(lone, middle_hat[1], b_imag)
                mirror_power = jnp.where(lone, middle_power, power)
            counted(group, power, mirror_power)
            hats_a.append(
                jnp.concatenate(
                    [kernel_real * real - odd * imag, kernel_real * imag + odd * real], axis=1
                )
            )
            hats_b.append(jnp.concatenate([b_real, b_imag], axis=1))
        for which, hats in enumerate((hats_a, hats_b)):
            restored = back(hats)
            for part in range(2):
                for side in range(2):
                    tile = 8 * part + 4 * which + 2 * pair + side
                    out_ref[pl.ds(tile, LONG, BACK), :] = restored[
                        LONG * part : LONG * part + LONG, LONG * side : LONG * side + LONG
                    ]

    row = lax.broadcasted_iota(jnp.int32, (LONG, NBINS), 0)
    column = lax.broadcasted_iota(jnp.int32, (LONG, NBINS), 1)
    sums = jnp.where(row % 8 == column % 8, bands_ref[...], 0.0)
    sums = jnp.sum(sums.reshape(2, 8, 8, NBINS).sum(axis=0), axis=1)
    left = lax.broadcasted_iota(jnp.int32, (NBINS, LONG), 0)
    right = lax.broadcasted_iota(jnp.int32, (NBINS, LONG), 1)
    gather = jnp.where((left // 8 == right % 8) & (right < NBINS), 1.0, 0.0)
    sums = lax.dot_general(
        sums,
        gather,
        (((1,), (0,)), ((), ())),
        precision=lax.Precision.HIGHEST,
        preferred_element_type=jnp.float32,
    )
    coarse = lax.broadcasted_iota(jnp.int32, (8, LONG), 0)
    lanes = lax.broadcasted_iota(jnp.int32, (8, LONG), 1)
    line = jnp.sum(jnp.where(lanes // 8 == coarse, sums, 0.0), axis=0, keepdims=True)
    line = line * (NBINS / float(N) ** 4)
    out_ref[pl.ds(16, LONG, BACK), :] = jnp.broadcast_to(line, (LONG, LONG))


def rows_back_kernel(
    arrived_ref, turn_ref, table_ref, real_ref, imag_ref, spectrum_ref, held_ref
):
    for group in range(8):
        pair = jnp.concatenate(
            [
                arrived_ref[pl.ds(group, LONG, BACK), :].T,
                arrived_ref[pl.ds(8 + group, LONG, BACK), :].T,
            ],
            axis=1,
        )
        held_ref[LONG * group : LONG * group + LONG, :] = times_table(pair, table_ref)
    bands = jnp.sum(arrived_ref[pl.ds(16, LONG, BACK), :], axis=0, keepdims=True)
    spectrum_ref[...] = bands[:, :NBINS]
    for block in range(4):
        pieces = [None] * SHORT
        for k in range(SHORT // 2):
            turned = []
            for which in range(2):
                start = SHORT * (SHORT // 2 * which + k) + 8 * block
                rows = slice(start, start + 8)
                turn = k + SHORT // 2 if which and not k else k
                cosine = turn_ref[0, turn : turn + 1, :]
                sine = turn_ref[1, turn : turn + 1, :]
                real, imag = held_ref[rows, :LONG], held_ref[rows, LONG:]
                turned.append((real * cosine - imag * sine, imag * cosine + real * sine))
            (a_real, a_imag), (b_real, b_imag) = turned
            if k == 0:
                pieces[0], pieces[SHORT // 2] = turned
            else:
                pieces[k] = (a_real - b_imag, a_imag + b_real)
                pieces[SHORT - k] = (a_real + b_imag, b_real - a_imag)
        for n, (real, imag) in enumerate(transformed(pieces, 1.0)):
            real_ref[8 * block : 8 * block + 8, LONG * n : LONG * n + LONG] = real
            imag_ref[8 * block : 8 * block + 8, LONG * n : LONG * n + LONG] = imag


def call(kernel, outs, scratch, inputs, smem_first=False):
    whole = pl.BlockSpec(memory_space=pltpu.VMEM)
    specs = [whole] * len(inputs)
    if smem_first:
        specs[0] = pl.BlockSpec(memory_space=pltpu.SMEM)
    return pl.pallas_call(
        kernel,
        out_shape=outs,
        in_specs=specs,
        out_specs=jax.tree.map(lambda _: whole, outs),
        scratch_shapes=scratch,
        compiler_params=pltpu.CompilerParams(vmem_limit_bytes=48 * 1024 * 1024),
    )(*inputs)


def f32(*shape):
    return jax.ShapeDtypeStruct(shape, jnp.float32)


def exchanged(array, height):
    blocks = array.reshape(LONG, 1, height * LONG)
    blocks = lax.all_to_all(blocks, ROWS_PLANES, split_axis=0, concat_axis=0, tiled=True)
    return blocks.reshape(LONG * height, LONG)


def along(array, step):
    return lax.ppermute(array, PLANES[0], [(i, (i + step) % 4) for i in range(4)])


def swapped(array):
    return lax.ppermute(array, PLANES[1], [(0, 1), (1, 0)])


def after(array, other):
    return lax.optimization_barrier((array, other))[0]


def plane_sum(density, weight):
    length = density.shape[-1]
    here = lax.axis_index(PLANES[0])
    upper = lax.axis_index(PLANES[1])
    blocks = density.reshape(4, 2, -1, length)
    rows = blocks.shape[2]

    def early(source, step, side):
        got = lax.dynamic_slice(
            source, ((here + step) & 3, 0, 0, side * EARLY_HALF), (1, 2, rows, EARLY_HALF)
        )
        return got[0] * weight

    def late_block(source, half):
        got = lax.dynamic_slice(source, (0, half, 0, EARLY), (4, 1, rows, length - EARLY))
        return got[:, 0] * weight

    far_up = along(early(blocks, 2, 0), 1)
    far_down = along(early(blocks, 2, 1), -1)
    late_sent = late_block(blocks, 1 - upper)
    late_other = swapped(late_sent)
    up_free = along(early(blocks, 1, 1), 1)
    down_free = along(early(blocks, -1, 0), -1)
    up_bound = along(early(after(blocks, far_up), 1, 0) + far_up, 1)
    down_bound = along(early(after(blocks, far_down), -1, 1) + far_down, -1)
    late = late_block(after(blocks, late_other), upper) + late_other

    def late_piece(step):
        return lax.dynamic_index_in_dim(late, (here + step) & 3, 0, keepdims=False)

    late_terms = [along(late_piece(step), step) for step in (1, -1, 2)]
    whole = after(blocks, up_bound)
    early_sum = jnp.concatenate(
        [
            early(whole, 0, 0) + up_bound + down_free,
            early(whole, 0, 1) + up_free + down_bound,
        ],
        axis=-1,
    )
    sent = lax.dynamic_index_in_dim(early_sum, 1 - upper, 0, keepdims=False)
    mine = lax.dynamic_index_in_dim(early_sum, upper, 0, keepdims=False)
    other = swapped(sent)
    return (mine, other, late_piece(0), *late_terms)


def tiled(columns):
    return columns.reshape(4, 4, SHORT, LONG).transpose(0, 3, 1, 2).reshape(4 * LONG, LONG)


def swapped_mirror(array):
    return lax.ppermute(array, ROWS_PLANES, [(i, LONG - 1 - i) for i in range(LONG)])


def on_device(density, lens_weight, spectrum_bin):
    held = tables()
    device = lax.axis_index(ROWS_PLANES)
    parts = plane_sum(density[0], lens_weight[0])
    columns = spectrum_bin.T
    mirrored = jnp.roll(columns[SHORT // 2 + 1 :, ::-1], 1, axis=1)[::-1]
    mirrored = tiled(jnp.concatenate([columns[:1], mirrored], axis=0))
    bins = tiled(columns[: SHORT // 2])
    middle = columns[SHORT // 2].reshape(SHORT, LONG).T
    middle = jnp.pad(middle, ((0, 0), (0, 3 * SHORT)))
    mirror = swapped_mirror(after(mirrored, parts[1]))
    sent = call(
        rows_forth_kernel,
        f32(LONG * FORTH, LONG),
        [pltpu.VMEM((SHORT, 4, 8, 2 * LONG), jnp.float32)],
        (*parts, held["row_turn"], held["forth"]),
    )
    arrived = exchanged(sent, FORTH)
    sent = call(
        columns_kernel,
        f32(LONG * BACK, LONG),
        [pltpu.VMEM((LONG, NBINS), jnp.float32)],
        (
            (device * SHORT).reshape(1),
            arrived,
            bins,
            mirror,
            middle,
            held["column_turn"],
            held["forth"],
            held["back"],
            held["short_forth"],
            held["short_back"],
        ),
        smem_first=True,
    )
    arrived = exchanged(sent, BACK)
    shear_real, shear_imag, spectrum = call(
        rows_back_kernel,
        (f32(SHORT, N), f32(SHORT, N), f32(1, NBINS)),
        [pltpu.VMEM((8 * LONG, 2 * LONG), jnp.float32)],
        (arrived, held["row_turn"], held["right_back"]),
    )
    return shear_real, shear_imag, spectrum[0]


def solution(mesh):
    finer = Mesh(mesh.devices.reshape(4, 2, 2, 4, 2), ROWS_PLANES)
    in_specs = (P(PLANES, ROWS, None), P(PLANES), P(None, ROWS_PLANES))
    out_specs = (P(ROWS_PLANES, None), P(ROWS_PLANES, None), P())
    return jax.shard_map(
        on_device, mesh=finer, in_specs=in_specs, out_specs=out_specs, check_vma=False
    )
```

```python
import math

import numpy as np
import jax
import jax.numpy as jnp
from jax import lax
from jax.experimental import pallas as pl
from jax.experimental.pallas import tpu as pltpu
from jax.sharding import Mesh
from jax.sharding import PartitionSpec as P


N = 4096
LONG = 128
SHORT = 32
NBINS = 64
ROWS = ("rows_0", "rows_1", "rows_2")
PLANES = ("planes_0", "planes_1")
ROWS_PLANES = ROWS + PLANES
FORTH = 9
BACK = 17
EARLY_HALF = 1280
EARLY = 2 * EARLY_HALF
BF16 = jnp.bfloat16


def halves(table):
    high = table.astype(np.float32).astype(jnp.bfloat16)
    low = (table - high.astype(np.float64)).astype(np.float32).astype(jnp.bfloat16)
    return high, low


def tables():
    def wave(left, right, length):
        angle = 2.0 * np.pi * ((left[:, None] * right[None, :]) % length) / length
        return np.cos(angle), np.sin(angle)

    long_index = np.arange(LONG)
    short_index = np.arange(SHORT)
    cos_long, sin_long = wave(long_index, long_index, LONG)
    forth = np.block([[cos_long, sin_long], [-sin_long, cos_long]])
    cos_short, sin_short = wave(short_index, short_index, SHORT)
    cos_four, sin_four = np.kron(np.eye(4), cos_short), np.kron(np.eye(4), sin_short)
    short_forth = np.block([[cos_four, -sin_four], [sin_four, cos_four]])
    row_turn = wave(short_index, long_index, N)
    cos_turn, sin_turn = wave(long_index, short_index, N)
    column_turn = (np.tile(cos_turn, (1, 4)), np.tile(sin_turn, (1, 4)))
    return {
        "forth": np.concatenate(halves(forth), axis=1),
        "back": np.concatenate(halves(forth.T), axis=1),
        "short_forth": np.concatenate(halves(short_forth), axis=0),
        "short_back": np.concatenate(halves(short_forth.T), axis=0),
        "right_back": np.concatenate(halves(forth), axis=0),
        "row_turn": np.stack(row_turn).astype(np.float32),
        "column_turn": np.stack(column_turn).astype(np.float32),
    }


def plus(a, b):
    if a is None:
        return b
    if b is None:
        return a
    return a + b


def minus(a, b):
    if b is None:
        return a
    if a is None:
        return -b
    return a - b


def scaled(a, factor):
    if a is None or factor == 0.0:
        return None
    if factor == 1.0:
        return a
    if factor == -1.0:
        return -a
    return a * factor


def rotated(value, step, length, orient):
    step %= length
    quarter, rest = divmod(4 * step, length)
    real, imag = value
    if rest == 0:
        cosine = (1.0, 0.0, -1.0, 0.0)[quarter]
        sine = (0.0, 1.0, 0.0, -1.0)[quarter] * orient
    else:
        cosine = math.cos(2.0 * math.pi * step / length)
        sine = orient * math.sin(2.0 * math.pi * step / length)
    return (
        minus(scaled(real, cosine), scaled(imag, sine)),
        plus(scaled(real, sine), scaled(imag, cosine)),
    )


def transformed(values, orient):
    length = len(values)
    if length == 1:
        return values
    even = transformed(values[0::2], orient)
    odd = transformed(values[1::2], orient)
    front, rear = [], []
    for k in range(length // 2):
        turned = rotated(odd[k], k, length, orient)
        front.append((plus(even[k][0], turned[0]), plus(even[k][1], turned[1])))
        rear.append((minus(even[k][0], turned[0]), minus(even[k][1], turned[1])))
    return front + rear


def transformed_real(values):
    length = len(values)
    if length == 1:
        return [(values[0], None)]
    if length == 2:
        return [(values[0] + values[1], None), (values[0] - values[1], None)]
    even = transformed_real(values[0::2])
    odd = transformed_real(values[1::2])
    out = [None] * (length // 2 + 1)
    for k in range(length // 4 + 1):
        turned = rotated(odd[k], k, length, -1.0)
        out[k] = (plus(even[k][0], turned[0]), plus(even[k][1], turned[1]))
        mirror_imag = minus(turned[1], even[k][1])
        out[length // 2 - k] = (minus(even[k][0], turned[0]), mirror_imag)
    return out


def split(value):
    high = value.astype(BF16)
    return high, (value - high.astype(jnp.float32)).astype(BF16)


def product(left, right, dims=((1,), (0,))):
    return lax.dot_general(left, right, (dims, ((), ())), preferred_element_type=jnp.float32)


def table_times(table_ref, value):
    size = value.shape[0]
    high, low = split(value)
    stacked = jnp.concatenate([high, low, high], axis=0)
    left = jnp.concatenate([table_ref[:, :size], table_ref[:, :size], table_ref[:, size:]], axis=1)
    return product(left, stacked)


def table_times_rows(table_ref, value):
    size = value.shape[1]
    high, low = split(value)
    stacked = jnp.concatenate([high, low, high], axis=1)
    left = jnp.concatenate([table_ref[:, :size], table_ref[:, :size], table_ref[:, size:]], axis=1)
    return product(left, stacked, ((1,), (1,)))


def times_table(value, table_ref):
    size = value.shape[1]
    high, low = split(value)
    stacked = jnp.concatenate([high, low, high], axis=1)
    right = jnp.concatenate([table_ref[:size], table_ref[:size], table_ref[size:]], axis=0)
    return product(stacked, right)


def rows_forth_kernel(*refs):
    field_refs = refs[:6]
    turn_ref, forth_ref, out_ref, held_ref = refs[6:]
    for block in range(4):
        rows = slice(8 * block, 8 * block + 8)
        pieces = []
        for n in range(SHORT):
            terms, start = part_terms(field_refs, LONG * n)
            lanes = slice(LONG * n - start, LONG * n - start + LONG)
            total = terms[0][rows, lanes]
            for term in terms[1:]:
                total = total + term[rows, lanes]
            pieces.append(total)
        for k, (real, imag) in enumerate(transformed_real(pieces)):
            cosine = turn_ref[0, k : k + 1, :]
            sine = turn_ref[1, k : k + 1, :]
            if imag is None:
                held_ref[k, block, :, :LONG] = real * cosine
                held_ref[k, block, :, LONG:] = -(real * sine)
            else:
                held_ref[k, block, :, :LONG] = real * cosine + imag * sine
                held_ref[k, block, :, LONG:] = imag * cosine - real * sine
    for half in range(2):
        rows = held_ref[8 * half : 8 * half + 8].reshape(256, 2 * LONG)
        spread = table_times_rows(forth_ref, rows)
        for part in range(2):
            for side in range(2):
                tile = 4 * part + 2 * half + side
                out_ref[pl.ds(tile, LONG, FORTH), :] = spread[
                    LONG * part : LONG * part + LONG, LONG * side : LONG * side + LONG
                ]
    last = held_ref[SHORT // 2].reshape(SHORT, 2 * LONG)
    real, imag = last[:, :LONG], last[:, LONG:]
    turned = jnp.concatenate([imag, -real], axis=1)
    nothing = jnp.zeros((2 * SHORT, 2 * LONG), jnp.float32)
    spread = table_times_rows(forth_ref, jnp.concatenate([last, turned, nothing], axis=0))
    out_ref[pl.ds(8, LONG, FORTH), :] = spread[:LONG]


def part_terms(refs, column):
    if column < EARLY:
        return refs[:2], 0
    return refs[2:6], EARLY


def columns_kernel(
    first_ref,
    arrived_ref,
    bins_ref,
    mirror_ref,
    middle_ref,
    turn_ref,
    forth_ref,
    back_ref,
    short_forth_ref,
    short_back_ref,
    out_ref,
    bands_ref,
):
    lane = lax.broadcasted_iota(jnp.int32, (LONG, LONG), 1)
    row = lax.broadcasted_iota(jnp.int32, (LONG, LONG), 0)
    height = row + LONG * (lane % SHORT)
    height = ((height + N // 2) % N - N // 2).astype(jnp.float32)
    height_square = height * height
    first = first_ref[0]
    cosine = turn_ref[0]
    sine = turn_ref[1]
    lone = lane < SHORT
    edge = height == -(N // 2)

    def forth(tiles):
        spread = table_times(
            forth_ref, jnp.concatenate([jnp.concatenate(tile, axis=0) for tile in tiles], axis=1)
        )
        turned = []
        for side in range(len(tiles)):
            lanes = slice(LONG * side, LONG * side + LONG)
            real, imag = spread[:LONG, lanes], spread[LONG:, lanes]
            turned.append(
                jnp.concatenate([real * cosine + imag * sine, imag * cosine - real * sine], axis=1)
            )
        held = times_table(jnp.concatenate(turned, axis=0), short_forth_ref)
        rows = [slice(LONG * side, LONG * side + LONG) for side in range(len(tiles))]
        return [(held[r, :LONG], held[r, LONG:]) for r in rows]

    def kernels(group, pair):
        real, imag = pair
        across = first + 4 * group + lane // SHORT
        across = ((across + N // 2) % N - N // 2).astype(jnp.float32)
        across_square = across * across
        square_norm = height_square + across_square
        anchor = square_norm == 0.0
        real = jnp.where(anchor, 0.0, real)
        imag = jnp.where(anchor, 0.0, imag)
        inverse = (1.0 / float(N) ** 2) / jnp.where(anchor, 1.0, square_norm)
        kernel_real = (across_square - height_square) * inverse
        kernel_imag = (across * height) * (2.0 * inverse)
        return real, imag, kernel_real, kernel_imag

    def back(hats):
        returned = times_table(jnp.concatenate(hats, axis=0), short_back_ref)
        columns = []
        for side in range(2):
            rows = slice(LONG * side, LONG * side + LONG)
            real, imag = returned[rows, :LONG], returned[rows, LONG:]
            columns.append(
                jnp.concatenate([real * cosine - imag * sine, imag * cosine + real * sine], axis=0)
            )
        return table_times(back_ref, jnp.concatenate(columns, axis=1))

    bands_ref[...] = jnp.zeros_like(bands_ref)

    def counted(group, power, mirror_power):
        rows = slice(LONG * group, LONG * group + LONG)
        mirror_bins = mirror_ref[rows]
        if group == 0:
            mirror_bins = jnp.where(lone, middle_ref[...], mirror_bins)
        for got, bins in ((power, bins_ref[rows]), (mirror_power, mirror_bins)):
            high = got.astype(BF16).astype(jnp.float32)
            low = got - high
            coarse, fine = bins >> 3, bins & 7
            values, marks = [], []
            for start in range(0, LONG, 8):
                here = slice(start, start + 8)
                chosen = [coarse[here] == index for index in range(8)]
                stack = [jnp.where(mask, high[here], 0.0) for mask in chosen]
                stack += [jnp.where(mask, low[here], 0.0) for mask in chosen]
                values.append(jnp.concatenate(stack, axis=0).astype(BF16))
                stack = [jnp.where(fine[here] == index, 1.0, 0.0) for index in range(8)]
                marks.append(jnp.concatenate(stack, axis=0).astype(BF16))
            bands_ref[...] += product(
                jnp.concatenate(values, axis=1), jnp.concatenate(marks, axis=1), ((1,), (1,))
            )

    middle = arrived_ref[pl.ds(8, LONG, FORTH), :]
    tile = (jnp.where(lone, middle, 0.0), jnp.where(lone, pltpu.roll(middle, 96, 1), 0.0))
    real, imag, kernel_real, kernel_imag = kernels(4, forth([tile])[0])
    middle_power = real * real + imag * imag
    middle_hat = (kernel_real * real - kernel_imag * imag, kernel_real * imag + kernel_imag * real)
    for pair in range(2):
        tiles = [
            (arrived_ref[pl.ds(g, LONG, FORTH), :], arrived_ref[pl.ds(4 + g, LONG, FORTH), :])
            for g in (2 * pair, 2 * pair + 1)
        ]
        hats_a, hats_b = [], []
        for side, got in enumerate(forth(tiles)):
            group = 2 * pair + side
            real, imag, kernel_real, kernel_imag = kernels(group, got)
            power = real * real + imag * imag
            single = edge | lone if group == 0 else edge
            odd = jnp.where(single, kernel_imag, 0.0)
            even = jnp.where(single, 0.0, kernel_imag)
            b_real, b_imag = even * real, even * imag
            mirror_power = power
            if group == 0:
                b_real = jnp.where(lone, middle_hat[0], b_real)
                b_imag = jnp.where(lone, middle_hat[1], b_imag)
                mirror_power = jnp.where(lone, middle_power, power)
            counted(group, power, mirror_power)
            hats_a.append(
                jnp.concatenate(
                    [kernel_real * real - odd * imag, kernel_real * imag + odd * real], axis=1
                )
            )
            hats_b.append(jnp.concatenate([b_real, b_imag], axis=1))
        for which, hats in enumerate((hats_a, hats_b)):
            restored = back(hats)
            for part in range(2):
                for side in range(2):
                    tile = 8 * part + 4 * which + 2 * pair + side
                    out_ref[pl.ds(tile, LONG, BACK), :] = restored[
                        LONG * part : LONG * part + LONG, LONG * side : LONG * side + LONG
                    ]

    row = lax.broadcasted_iota(jnp.int32, (LONG, NBINS), 0)
    column = lax.broadcasted_iota(jnp.int32, (LONG, NBINS), 1)
    sums = jnp.where(row % 8 == column % 8, bands_ref[...], 0.0)
    sums = jnp.sum(sums.reshape(2, 8, 8, NBINS).sum(axis=0), axis=1)
    left = lax.broadcasted_iota(jnp.int32, (NBINS, LONG), 0)
    right = lax.broadcasted_iota(jnp.int32, (NBINS, LONG), 1)
    gather = jnp.where((left // 8 == right % 8) & (right < NBINS), 1.0, 0.0)
    sums = lax.dot_general(
        sums,
        gather,
        (((1,), (0,)), ((), ())),
        precision=lax.Precision.HIGHEST,
        preferred_element_type=jnp.float32,
    )
    coarse = lax.broadcasted_iota(jnp.int32, (8, LONG), 0)
    lanes = lax.broadcasted_iota(jnp.int32, (8, LONG), 1)
    line = jnp.sum(jnp.where(lanes // 8 == coarse, sums, 0.0), axis=0, keepdims=True)
    line = line * (NBINS / float(N) ** 4)
    out_ref[pl.ds(16, LONG, BACK), :] = jnp.broadcast_to(line, (LONG, LONG))


def rows_back_kernel(
    arrived_ref, turn_ref, table_ref, real_ref, imag_ref, spectrum_ref, held_ref
):
    for group in range(8):
        pair = jnp.concatenate(
            [
                arrived_ref[pl.ds(group, LONG, BACK), :].T,
                arrived_ref[pl.ds(8 + group, LONG, BACK), :].T,
            ],
            axis=1,
        )
        held_ref[LONG * group : LONG * group + LONG, :] = times_table(pair, table_ref)
    bands = jnp.sum(arrived_ref[pl.ds(16, LONG, BACK), :], axis=0, keepdims=True)
    spectrum_ref[...] = bands[:, :NBINS]
    for block in range(4):
        pieces = [None] * SHORT
        for k in range(SHORT // 2):
            turned = []
            for which in range(2):
                start = SHORT * (SHORT // 2 * which + k) + 8 * block
                rows = slice(start, start + 8)
                turn = k + SHORT // 2 if which and not k else k
                cosine = turn_ref[0, turn : turn + 1, :]
                sine = turn_ref[1, turn : turn + 1, :]
                real, imag = held_ref[rows, :LONG], held_ref[rows, LONG:]
                turned.append((real * cosine - imag * sine, imag * cosine + real * sine))
            (a_real, a_imag), (b_real, b_imag) = turned
            if k == 0:
                pieces[0], pieces[SHORT // 2] = turned
            else:
                pieces[k] = (a_real - b_imag, a_imag + b_real)
                pieces[SHORT - k] = (a_real + b_imag, b_real - a_imag)
        for n, (real, imag) in enumerate(transformed(pieces, 1.0)):
            real_ref[8 * block : 8 * block + 8, LONG * n : LONG * n + LONG] = real
            imag_ref[8 * block : 8 * block + 8, LONG * n : LONG * n + LONG] = imag


def call(kernel, outs, scratch, inputs, smem_first=False):
    whole = pl.BlockSpec(memory_space=pltpu.VMEM)
    specs = [whole] * len(inputs)
    if smem_first:
        specs[0] = pl.BlockSpec(memory_space=pltpu.SMEM)
    return pl.pallas_call(
        kernel,
        out_shape=outs,
        in_specs=specs,
        out_specs=jax.tree.map(lambda _: whole, outs),
        scratch_shapes=scratch,
        compiler_params=pltpu.CompilerParams(vmem_limit_bytes=48 * 1024 * 1024),
    )(*inputs)


def f32(*shape):
    return jax.ShapeDtypeStruct(shape, jnp.float32)


def exchanged(array, height):
    blocks = array.reshape(LONG, 1, height * LONG)
    blocks = lax.all_to_all(blocks, ROWS_PLANES, split_axis=0, concat_axis=0, tiled=True)
    return blocks.reshape(LONG * height, LONG)


def along(array, step):
    return lax.ppermute(array, PLANES[0], [(i, (i + step) % 4) for i in range(4)])


def swapped(array):
    return lax.ppermute(array, PLANES[1], [(0, 1), (1, 0)])


def after(array, other):
    return lax.optimization_barrier((array, other))[0]


def plane_sum(density, weight):
    length = density.shape[-1]
    here = lax.axis_index(PLANES[0])
    upper = lax.axis_index(PLANES[1])
    blocks = density.reshape(4, 2, -1, length)
    rows = blocks.shape[2]

    def early(source, step, side):
        got = lax.dynamic_slice(
            source, ((here + step) & 3, 0, 0, side * EARLY_HALF), (1, 2, rows, EARLY_HALF)
        )
        return got[0] * weight

    def late_block(source, half):
        got = lax.dynamic_slice(source, (0, half, 0, EARLY), (4, 1, rows, length - EARLY))
        return got[:, 0] * weight

    far_pieces = early(blocks, 2, 0), early(blocks, 2, 1)
    far_up = along(far_pieces[0], 1)
    far_down = along(far_pieces[1], -1)
    behind = after(blocks, far_pieces[0])
    late_sent = late_block(behind, 1 - upper)
    late_other = swapped(late_sent)
    up_free = along(early(behind, 1, 1), 1)
    down_free = along(early(behind, -1, 0), -1)
    up_bound = along(early(after(blocks, far_up), 1, 0) + far_up, 1)
    down_bound = along(early(after(blocks, far_down), -1, 1) + far_down, -1)
    late = late_block(after(blocks, late_other), upper) + late_other

    def late_piece(step):
        return lax.dynamic_index_in_dim(late, (here + step) & 3, 0, keepdims=False)

    late_terms = [along(late_piece(step), step) for step in (1, -1, 2)]
    whole = after(blocks, up_bound)
    early_sum = jnp.concatenate(
        [
            early(whole, 0, 0) + up_bound + down_free,
            early(whole, 0, 1) + up_free + down_bound,
        ],
        axis=-1,
    )
    sent = lax.dynamic_index_in_dim(early_sum, 1 - upper, 0, keepdims=False)
    mine = lax.dynamic_index_in_dim(early_sum, upper, 0, keepdims=False)
    other = swapped(sent)
    return (mine, other, late_piece(0), *late_terms)


def tiled(columns):
    return columns.reshape(4, 4, SHORT, LONG).transpose(0, 3, 1, 2).reshape(4 * LONG, LONG)


def swapped_mirror(array):
    return lax.ppermute(array, ROWS_PLANES, [(i, LONG - 1 - i) for i in range(LONG)])


def on_device(density, lens_weight, spectrum_bin):
    held = tables()
    device = lax.axis_index(ROWS_PLANES)
    parts = plane_sum(density[0], lens_weight[0])
    columns = spectrum_bin.T
    mirrored = jnp.roll(columns[SHORT // 2 + 1 :, ::-1], 1, axis=1)[::-1]
    mirrored = tiled(jnp.concatenate([columns[:1], mirrored], axis=0))
    bins = tiled(columns[: SHORT // 2])
    middle = columns[SHORT // 2].reshape(SHORT, LONG).T
    middle = jnp.pad(middle, ((0, 0), (0, 3 * SHORT)))
    mirror = swapped_mirror(mirrored)
    sent = call(
        rows_forth_kernel,
        f32(LONG * FORTH, LONG),
        [pltpu.VMEM((SHORT, 4, 8, 2 * LONG), jnp.float32)],
        (*parts, held["row_turn"], held["forth"]),
    )
    arrived = exchanged(sent, FORTH)
    sent = call(
        columns_kernel,
        f32(LONG * BACK, LONG),
        [pltpu.VMEM((LONG, NBINS), jnp.float32)],
        (
            (device * SHORT).reshape(1),
            arrived,
            bins,
            mirror,
            middle,
            held["column_turn"],
            held["forth"],
            held["back"],
            held["short_forth"],
            held["short_back"],
        ),
        smem_first=True,
    )
    arrived = exchanged(sent, BACK)
    shear_real, shear_imag, spectrum = call(
        rows_back_kernel,
        (f32(SHORT, N), f32(SHORT, N), f32(1, NBINS)),
        [pltpu.VMEM((8 * LONG, 2 * LONG), jnp.float32)],
        (arrived, held["row_turn"], held["right_back"]),
    )
    return shear_real, shear_imag, spectrum[0]


def solution(mesh):
    finer = Mesh(mesh.devices.reshape(4, 2, 2, 4, 2), ROWS_PLANES)
    in_specs = (P(PLANES, ROWS, None), P(PLANES), P(None, ROWS_PLANES))
    out_specs = (P(ROWS_PLANES, None), P(ROWS_PLANES, None), P())
    return jax.shard_map(
        on_device, mesh=finer, in_specs=in_specs, out_specs=out_specs, check_vma=False
    )
```

```python
import math

import numpy as np
import jax
import jax.numpy as jnp
from jax import lax
from jax.experimental import pallas as pl
from jax.experimental.pallas import tpu as pltpu
from jax.sharding import Mesh
from jax.sharding import PartitionSpec as P


N = 4096
LONG = 128
SHORT = 32
NBINS = 64
ROWS = ("rows_0", "rows_1", "rows_2")
PLANES = ("planes_0", "planes_1")
ROWS_PLANES = ROWS + PLANES
FORTH = 9
BACK = 17
EARLY_HALF = 1152
EARLY = 2 * EARLY_HALF
BF16 = jnp.bfloat16


def halves(table):
    high = table.astype(np.float32).astype(jnp.bfloat16)
    low = (table - high.astype(np.float64)).astype(np.float32).astype(jnp.bfloat16)
    return high, low


def tables():
    def wave(left, right, length):
        angle = 2.0 * np.pi * ((left[:, None] * right[None, :]) % length) / length
        return np.cos(angle), np.sin(angle)

    long_index = np.arange(LONG)
    short_index = np.arange(SHORT)
    cos_long, sin_long = wave(long_index, long_index, LONG)
    forth = np.block([[cos_long, sin_long], [-sin_long, cos_long]])
    cos_short, sin_short = wave(short_index, short_index, SHORT)
    cos_four, sin_four = np.kron(np.eye(4), cos_short), np.kron(np.eye(4), sin_short)
    short_forth = np.block([[cos_four, -sin_four], [sin_four, cos_four]])
    row_turn = wave(short_index, long_index, N)
    cos_turn, sin_turn = wave(long_index, short_index, N)
    column_turn = (np.tile(cos_turn, (1, 4)), np.tile(sin_turn, (1, 4)))
    return {
        "forth": np.concatenate(halves(forth), axis=1),
        "back": np.concatenate(halves(forth.T), axis=1),
        "short_forth": np.concatenate(halves(short_forth), axis=0),
        "short_back": np.concatenate(halves(short_forth.T), axis=0),
        "right_back": np.concatenate(halves(forth), axis=0),
        "row_turn": np.stack(row_turn).astype(np.float32),
        "column_turn": np.stack(column_turn).astype(np.float32),
    }


def plus(a, b):
    if a is None:
        return b
    if b is None:
        return a
    return a + b


def minus(a, b):
    if b is None:
        return a
    if a is None:
        return -b
    return a - b


def scaled(a, factor):
    if a is None or factor == 0.0:
        return None
    if factor == 1.0:
        return a
    if factor == -1.0:
        return -a
    return a * factor


def rotated(value, step, length, orient):
    step %= length
    quarter, rest = divmod(4 * step, length)
    real, imag = value
    if rest == 0:
        cosine = (1.0, 0.0, -1.0, 0.0)[quarter]
        sine = (0.0, 1.0, 0.0, -1.0)[quarter] * orient
    else:
        cosine = math.cos(2.0 * math.pi * step / length)
        sine = orient * math.sin(2.0 * math.pi * step / length)
    return (
        minus(scaled(real, cosine), scaled(imag, sine)),
        plus(scaled(real, sine), scaled(imag, cosine)),
    )


def transformed(values, orient):
    length = len(values)
    if length == 1:
        return values
    even = transformed(values[0::2], orient)
    odd = transformed(values[1::2], orient)
    front, rear = [], []
    for k in range(length // 2):
        turned = rotated(odd[k], k, length, orient)
        front.append((plus(even[k][0], turned[0]), plus(even[k][1], turned[1])))
        rear.append((minus(even[k][0], turned[0]), minus(even[k][1], turned[1])))
    return front + rear


def transformed_real(values):
    length = len(values)
    if length == 1:
        return [(values[0], None)]
    if length == 2:
        return [(values[0] + values[1], None), (values[0] - values[1], None)]
    even = transformed_real(values[0::2])
    odd = transformed_real(values[1::2])
    out = [None] * (length // 2 + 1)
    for k in range(length // 4 + 1):
        turned = rotated(odd[k], k, length, -1.0)
        out[k] = (plus(even[k][0], turned[0]), plus(even[k][1], turned[1]))
        mirror_imag = minus(turned[1], even[k][1])
        out[length // 2 - k] = (minus(even[k][0], turned[0]), mirror_imag)
    return out


def split(value):
    high = value.astype(BF16)
    return high, (value - high.astype(jnp.float32)).astype(BF16)


def product(left, right, dims=((1,), (0,))):
    return lax.dot_general(left, right, (dims, ((), ())), preferred_element_type=jnp.float32)


def table_times(table_ref, value):
    size = value.shape[0]
    high, low = split(value)
    stacked = jnp.concatenate([high, low, high], axis=0)
    left = jnp.concatenate([table_ref[:, :size], table_ref[:, :size], table_ref[:, size:]], axis=1)
    return product(left, stacked)


def table_times_rows(table_ref, value):
    size = value.shape[1]
    high, low = split(value)
    stacked = jnp.concatenate([high, low, high], axis=1)
    left = jnp.concatenate([table_ref[:, :size], table_ref[:, :size], table_ref[:, size:]], axis=1)
    return product(left, stacked, ((1,), (1,)))


def times_table(value, table_ref):
    size = value.shape[1]
    high, low = split(value)
    stacked = jnp.concatenate([high, low, high], axis=1)
    right = jnp.concatenate([table_ref[:size], table_ref[:size], table_ref[size:]], axis=0)
    return product(stacked, right)


def rows_forth_kernel(*refs):
    field_refs = refs[:6]
    turn_ref, forth_ref, out_ref, held_ref = refs[6:]
    for block in range(4):
        rows = slice(8 * block, 8 * block + 8)
        pieces = []
        for n in range(SHORT):
            terms, start = part_terms(field_refs, LONG * n)
            lanes = slice(LONG * n - start, LONG * n - start + LONG)
            total = terms[0][rows, lanes]
            for term in terms[1:]:
                total = total + term[rows, lanes]
            pieces.append(total)
        for k, (real, imag) in enumerate(transformed_real(pieces)):
            cosine = turn_ref[0, k : k + 1, :]
            sine = turn_ref[1, k : k + 1, :]
            if imag is None:
                held_ref[k, block, :, :LONG] = real * cosine
                held_ref[k, block, :, LONG:] = -(real * sine)
            else:
                held_ref[k, block, :, :LONG] = real * cosine + imag * sine
                held_ref[k, block, :, LONG:] = imag * cosine - real * sine
    for half in range(2):
        rows = held_ref[8 * half : 8 * half + 8].reshape(256, 2 * LONG)
        spread = table_times_rows(forth_ref, rows)
        for part in range(2):
            for side in range(2):
                tile = 4 * part + 2 * half + side
                out_ref[pl.ds(tile, LONG, FORTH), :] = spread[
                    LONG * part : LONG * part + LONG, LONG * side : LONG * side + LONG
                ]
    last = held_ref[SHORT // 2].reshape(SHORT, 2 * LONG)
    real, imag = last[:, :LONG], last[:, LONG:]
    turned = jnp.concatenate([imag, -real], axis=1)
    nothing = jnp.zeros((2 * SHORT, 2 * LONG), jnp.float32)
    spread = table_times_rows(forth_ref, jnp.concatenate([last, turned, nothing], axis=0))
    out_ref[pl.ds(8, LONG, FORTH), :] = spread[:LONG]


def part_terms(refs, column):
    if column < EARLY:
        return refs[:2], 0
    return refs[2:6], EARLY


def columns_kernel(
    first_ref,
    arrived_ref,
    bins_ref,
    mirror_ref,
    middle_ref,
    turn_ref,
    forth_ref,
    back_ref,
    short_forth_ref,
    short_back_ref,
    out_ref,
    bands_ref,
):
    lane = lax.broadcasted_iota(jnp.int32, (LONG, LONG), 1)
    row = lax.broadcasted_iota(jnp.int32, (LONG, LONG), 0)
    height = row + LONG * (lane % SHORT)
    height = ((height + N // 2) % N - N // 2).astype(jnp.float32)
    height_square = height * height
    first = first_ref[0]
    cosine = turn_ref[0]
    sine = turn_ref[1]
    lone = lane < SHORT
    edge = height == -(N // 2)

    def forth(tiles):
        spread = table_times(
            forth_ref, jnp.concatenate([jnp.concatenate(tile, axis=0) for tile in tiles], axis=1)
        )
        turned = []
        for side in range(len(tiles)):
            lanes = slice(LONG * side, LONG * side + LONG)
            real, imag = spread[:LONG, lanes], spread[LONG:, lanes]
            turned.append(
                jnp.concatenate([real * cosine + imag * sine, imag * cosine - real * sine], axis=1)
            )
        held = times_table(jnp.concatenate(turned, axis=0), short_forth_ref)
        rows = [slice(LONG * side, LONG * side + LONG) for side in range(len(tiles))]
        return [(held[r, :LONG], held[r, LONG:]) for r in rows]

    def kernels(group, pair):
        real, imag = pair
        across = first + 4 * group + lane // SHORT
        across = ((across + N // 2) % N - N // 2).astype(jnp.float32)
        across_square = across * across
        square_norm = height_square + across_square
        anchor = square_norm == 0.0
        real = jnp.where(anchor, 0.0, real)
        imag = jnp.where(anchor, 0.0, imag)
        inverse = (1.0 / float(N) ** 2) / jnp.where(anchor, 1.0, square_norm)
        kernel_real = (across_square - height_square) * inverse
        kernel_imag = (across * height) * (2.0 * inverse)
        return real, imag, kernel_real, kernel_imag

    def back(hats):
        returned = times_table(jnp.concatenate(hats, axis=0), short_back_ref)
        columns = []
        for side in range(2):
            rows = slice(LONG * side, LONG * side + LONG)
            real, imag = returned[rows, :LONG], returned[rows, LONG:]
            columns.append(
                jnp.concatenate([real * cosine - imag * sine, imag * cosine + real * sine], axis=0)
            )
        return table_times(back_ref, jnp.concatenate(columns, axis=1))

    bands_ref[...] = jnp.zeros_like(bands_ref)

    def counted(group, power, mirror_power):
        rows = slice(LONG * group, LONG * group + LONG)
        mirror_bins = mirror_ref[rows]
        if group == 0:
            mirror_bins = jnp.where(lone, middle_ref[...], mirror_bins)
        for got, bins in ((power, bins_ref[rows]), (mirror_power, mirror_bins)):
            high = got.astype(BF16).astype(jnp.float32)
            low = got - high
            coarse, fine = bins >> 3, bins & 7
            values, marks = [], []
            for start in range(0, LONG, 8):
                here = slice(start, start + 8)
                chosen = [coarse[here] == index for index in range(8)]
                stack = [jnp.where(mask, high[here], 0.0) for mask in chosen]
                stack += [jnp.where(mask, low[here], 0.0) for mask in chosen]
                values.append(jnp.concatenate(stack, axis=0).astype(BF16))
                stack = [jnp.where(fine[here] == index, 1.0, 0.0) for index in range(8)]
                marks.append(jnp.concatenate(stack, axis=0).astype(BF16))
            bands_ref[...] += product(
                jnp.concatenate(values, axis=1), jnp.concatenate(marks, axis=1), ((1,), (1,))
            )

    middle = arrived_ref[pl.ds(8, LONG, FORTH), :]
    tile = (jnp.where(lone, middle, 0.0), jnp.where(lone, pltpu.roll(middle, 96, 1), 0.0))
    real, imag, kernel_real, kernel_imag = kernels(4, forth([tile])[0])
    middle_power = real * real + imag * imag
    middle_hat = (kernel_real * real - kernel_imag * imag, kernel_real * imag + kernel_imag * real)
    for pair in range(2):
        tiles = [
            (arrived_ref[pl.ds(g, LONG, FORTH), :], arrived_ref[pl.ds(4 + g, LONG, FORTH), :])
            for g in (2 * pair, 2 * pair + 1)
        ]
        hats_a, hats_b = [], []
        for side, got in enumerate(forth(tiles)):
            group = 2 * pair + side
            real, imag, kernel_real, kernel_imag = kernels(group, got)
            power = real * real + imag * imag
            single = edge | lone if group == 0 else edge
            odd = jnp.where(single, kernel_imag, 0.0)
            even = jnp.where(single, 0.0, kernel_imag)
            b_real, b_imag = even * real, even * imag
            mirror_power = power
            if group == 0:
                b_real = jnp.where(lone, middle_hat[0], b_real)
                b_imag = jnp.where(lone, middle_hat[1], b_imag)
                mirror_power = jnp.where(lone, middle_power, power)
            counted(group, power, mirror_power)
            hats_a.append(
                jnp.concatenate(
                    [kernel_real * real - odd * imag, kernel_real * imag + odd * real], axis=1
                )
            )
            hats_b.append(jnp.concatenate([b_real, b_imag], axis=1))
        for which, hats in enumerate((hats_a, hats_b)):
            restored = back(hats)
            for part in range(2):
                for side in range(2):
                    tile = 8 * part + 4 * which + 2 * pair + side
                    out_ref[pl.ds(tile, LONG, BACK), :] = restored[
                        LONG * part : LONG * part + LONG, LONG * side : LONG * side + LONG
                    ]

    row = lax.broadcasted_iota(jnp.int32, (LONG, NBINS), 0)
    column = lax.broadcasted_iota(jnp.int32, (LONG, NBINS), 1)
    sums = jnp.where(row % 8 == column % 8, bands_ref[...], 0.0)
    sums = jnp.sum(sums.reshape(2, 8, 8, NBINS).sum(axis=0), axis=1)
    left = lax.broadcasted_iota(jnp.int32, (NBINS, LONG), 0)
    right = lax.broadcasted_iota(jnp.int32, (NBINS, LONG), 1)
    gather = jnp.where((left // 8 == right % 8) & (right < NBINS), 1.0, 0.0)
    sums = lax.dot_general(
        sums,
        gather,
        (((1,), (0,)), ((), ())),
        precision=lax.Precision.HIGHEST,
        preferred_element_type=jnp.float32,
    )
    coarse = lax.broadcasted_iota(jnp.int32, (8, LONG), 0)
    lanes = lax.broadcasted_iota(jnp.int32, (8, LONG), 1)
    line = jnp.sum(jnp.where(lanes // 8 == coarse, sums, 0.0), axis=0, keepdims=True)
    line = line * (NBINS / float(N) ** 4)
    out_ref[pl.ds(16, LONG, BACK), :] = jnp.broadcast_to(line, (LONG, LONG))


def rows_back_kernel(
    arrived_ref, turn_ref, table_ref, real_ref, imag_ref, spectrum_ref, held_ref
):
    for group in range(8):
        pair = jnp.concatenate(
            [
                arrived_ref[pl.ds(group, LONG, BACK), :].T,
                arrived_ref[pl.ds(8 + group, LONG, BACK), :].T,
            ],
            axis=1,
        )
        held_ref[LONG * group : LONG * group + LONG, :] = times_table(pair, table_ref)
    bands = jnp.sum(arrived_ref[pl.ds(16, LONG, BACK), :], axis=0, keepdims=True)
    spectrum_ref[...] = bands[:, :NBINS]
    for block in range(4):
        pieces = [None] * SHORT
        for k in range(SHORT // 2):
            turned = []
            for which in range(2):
                start = SHORT * (SHORT // 2 * which + k) + 8 * block
                rows = slice(start, start + 8)
                turn = k + SHORT // 2 if which and not k else k
                cosine = turn_ref[0, turn : turn + 1, :]
                sine = turn_ref[1, turn : turn + 1, :]
                real, imag = held_ref[rows, :LONG], held_ref[rows, LONG:]
                turned.append((real * cosine - imag * sine, imag * cosine + real * sine))
            (a_real, a_imag), (b_real, b_imag) = turned
            if k == 0:
                pieces[0], pieces[SHORT // 2] = turned
            else:
                pieces[k] = (a_real - b_imag, a_imag + b_real)
                pieces[SHORT - k] = (a_real + b_imag, b_real - a_imag)
        for n, (real, imag) in enumerate(transformed(pieces, 1.0)):
            real_ref[8 * block : 8 * block + 8, LONG * n : LONG * n + LONG] = real
            imag_ref[8 * block : 8 * block + 8, LONG * n : LONG * n + LONG] = imag


def call(kernel, outs, scratch, inputs, smem_first=False):
    whole = pl.BlockSpec(memory_space=pltpu.VMEM)
    specs = [whole] * len(inputs)
    if smem_first:
        specs[0] = pl.BlockSpec(memory_space=pltpu.SMEM)
    return pl.pallas_call(
        kernel,
        out_shape=outs,
        in_specs=specs,
        out_specs=jax.tree.map(lambda _: whole, outs),
        scratch_shapes=scratch,
        compiler_params=pltpu.CompilerParams(vmem_limit_bytes=48 * 1024 * 1024),
    )(*inputs)


def f32(*shape):
    return jax.ShapeDtypeStruct(shape, jnp.float32)


def exchanged(array, height):
    blocks = array.reshape(LONG, 1, height * LONG)
    blocks = lax.all_to_all(blocks, ROWS_PLANES, split_axis=0, concat_axis=0, tiled=True)
    return blocks.reshape(LONG * height, LONG)


def along(array, step):
    return lax.ppermute(array, PLANES[0], [(i, (i + step) % 4) for i in range(4)])


def swapped(array):
    return lax.ppermute(array, PLANES[1], [(0, 1), (1, 0)])


def after(array, other):
    return lax.optimization_barrier((array, other))[0]


def plane_sum(density, weight):
    length = density.shape[-1]
    here = lax.axis_index(PLANES[0])
    upper = lax.axis_index(PLANES[1])
    blocks = density.reshape(4, 2, -1, length)
    rows = blocks.shape[2]

    def early(source, step, side):
        got = lax.dynamic_slice(
            source, ((here + step) & 3, 0, 0, side * EARLY_HALF), (1, 2, rows, EARLY_HALF)
        )
        return got[0] * weight

    def late_block(source, half):
        got = lax.dynamic_slice(source, (0, half, 0, EARLY), (4, 1, rows, length - EARLY))
        return got[:, 0] * weight

    late_sent = late_block(blocks, 1 - upper)
    front = after(blocks, late_sent)
    far_pieces = early(front, 2, 0), early(front, 2, 1)
    far_up = along(far_pieces[0], 1)
    far_down = along(far_pieces[1], -1)
    behind = after(blocks, far_pieces[0])
    late_other = swapped(late_sent)
    up_free = along(early(behind, 1, 1), 1)
    down_free = along(early(behind, -1, 0), -1)
    up_bound = along(early(after(blocks, far_up), 1, 0) + far_up, 1)
    down_bound = along(early(after(blocks, far_down), -1, 1) + far_down, -1)
    late = late_block(after(blocks, late_other), upper) + late_other

    def late_piece(step):
        return lax.dynamic_index_in_dim(late, (here + step) & 3, 0, keepdims=False)

    late_terms = [along(late_piece(step), step) for step in (1, -1, 2)]
    whole = after(blocks, up_bound)
    early_sum = jnp.concatenate(
        [
            early(whole, 0, 0) + up_bound + down_free,
            early(whole, 0, 1) + up_free + down_bound,
        ],
        axis=-1,
    )
    sent = lax.dynamic_index_in_dim(early_sum, 1 - upper, 0, keepdims=False)
    mine = lax.dynamic_index_in_dim(early_sum, upper, 0, keepdims=False)
    other = swapped(sent)
    return (mine, other, late_piece(0), *late_terms)


def tiled(columns):
    return columns.reshape(4, 4, SHORT, LONG).transpose(0, 3, 1, 2).reshape(4 * LONG, LONG)


def swapped_mirror(array):
    return lax.ppermute(array, ROWS_PLANES, [(i, LONG - 1 - i) for i in range(LONG)])


def on_device(density, lens_weight, spectrum_bin):
    held = tables()
    device = lax.axis_index(ROWS_PLANES)
    parts = plane_sum(density[0], lens_weight.reshape(1, 1, 1))
    columns = spectrum_bin.T
    mirrored = jnp.roll(columns[SHORT // 2 + 1 :, ::-1], 1, axis=1)[::-1]
    mirrored = tiled(jnp.concatenate([columns[:1], mirrored], axis=0))
    bins = tiled(columns[: SHORT // 2])
    middle = columns[SHORT // 2].reshape(SHORT, LONG).T
    middle = jnp.pad(middle, ((0, 0), (0, 3 * SHORT)))
    mirror = swapped_mirror(mirrored)
    sent = call(
        rows_forth_kernel,
        f32(LONG * FORTH, LONG),
        [pltpu.VMEM((SHORT, 4, 8, 2 * LONG), jnp.float32)],
        (*parts, held["row_turn"], held["forth"]),
    )
    arrived = exchanged(sent, FORTH)
    sent = call(
        columns_kernel,
        f32(LONG * BACK, LONG),
        [pltpu.VMEM((LONG, NBINS), jnp.float32)],
        (
            (device * SHORT).reshape(1),
            arrived,
            bins,
            mirror,
            middle,
            held["column_turn"],
            held["forth"],
            held["back"],
            held["short_forth"],
            held["short_back"],
        ),
        smem_first=True,
    )
    arrived = exchanged(sent, BACK)
    shear_real, shear_imag, spectrum = call(
        rows_back_kernel,
        (f32(SHORT, N), f32(SHORT, N), f32(1, NBINS)),
        [pltpu.VMEM((8 * LONG, 2 * LONG), jnp.float32)],
        (arrived, held["row_turn"], held["right_back"]),
    )
    return shear_real, shear_imag, spectrum[0]


def solution(mesh):
    finer = Mesh(mesh.devices.reshape(4, 2, 2, 4, 2), ROWS_PLANES)
    in_specs = (P(PLANES, ROWS, None), P(PLANES), P(None, ROWS_PLANES))
    out_specs = (P(ROWS_PLANES, None), P(ROWS_PLANES, None), P())
    return jax.shard_map(
        on_device, mesh=finer, in_specs=in_specs, out_specs=out_specs, check_vma=False
    )
```
